32 devices in a mesh: expert: 8 (over z, x), dp: 4 (over y, core).
Axes of the slice: x: 2, y: 2, z: 4, core: 2. Of those that a mesh axis runs over, the one named last changes fastest.
Arguments:
- tokens: bfloat16 [8192, 5120], P(('dp', 'expert')), parts along dimension 0, may hold values from -6 to 6
- router_logit: float32 [8192], P(('dp', 'expert')), parts along dimension 0, may hold values from 0 to 3
- expert_id: int32 [8192], P(('dp', 'expert')), parts along dimension 0, may hold values from 0 to 7, as said below
- token_slot: int32 [8192], P(('dp', 'expert')), parts along dimension 0, may hold values from 0 to 63, as said below
- keep: int32 [8192], P(('dp', 'expert')), parts along dimension 0, may hold values 0 or 1
- overflow_host: int32 [8, 32], replicated, may hold values from 0 to 7, as said below
- expert_gate: bfloat16 [8, 5120, 256], P('expert'), may hold values from -0.125 to 0.125
- expert_up: bfloat16 [8, 5120, 256], P('expert'), may hold values from -0.125 to 0.125
- expert_down: bfloat16 [8, 256, 5120], P('expert'), may hold values from -0.375 to 0.375
- shared_gate: bfloat16 [5120, 64], replicated, may hold values from -0.078125 to 0.078125
- shared_up: bfloat16 [5120, 64], replicated, may hold values from -0.078125 to 0.078125
- shared_down: bfloat16 [64, 5120], replicated, may hold values from -0.1875 to 0.1875
Outputs:
- moe_out: bfloat16 [8192, 5120], P(('dp', 'expert')), parts along dimension 0
The draws below stay inside these ranges and needn't reach their ends.
There are 4 independent parts, one for each index of `dp`. The reference program is written for one: setup_inputs(seed, part) draws one part's arguments, and reference() takes and returns one part's arrays. A program takes and returns all parts, laid end to end along the dimension named above; an argument that names none is the same for every part. Nothing has to cross between parts.
Inputs may be any that keep to these rules, and one draw needn't show every extreme that they name: `expert_id`: among the 256 tokens of one device at most 64 name the same expert; some experts are named by exactly 64 tokens of every device. `token_slot`: if c tokens of one device name the same expert, their slots are 0 to c - 1, each once. overflow_host[e, j] is e + 1 or e - 1, taken modulo 8.
All inputs are finite; a program needn't handle non-finite values. No bound on the sum of `keep` on one device may be relied on, other than what follows from the above.
Results may differ from the reference program's by a relative error of at most 0.007.
Values may be sent and summed in bfloat16 or wider, within the bound.
A program may use at most 128 MiB of HBM per device.

```python
import jax
import jax.numpy as jnp
from jax import lax

D = 5120
F = 256
SH = 64
T_DEV = 256
EXPERTS = 8
TOKENS = 2048
SLOTS = 64
HOME = 32
SPILL = 32


def draw_tokens(key, part):
    base_key = jax.random.fold_in(key, 31)
    key_row, key_value = jax.random.split(base_key, 2)
    values = jnp.clip(jax.random.normal(key_value, (TOKENS, D), jnp.float32), -6.0, 6.0)
    return values.astype(jnp.bfloat16)


def routing_pair(key):
    base_key = jax.random.fold_in(key, 11)
    key_hot, key_score, key_order = jax.random.split(base_key, 3)
    devices = TOKENS // T_DEV
    cell_count = EXPERTS * SLOTS
    hot_count = max(1, EXPERTS // 8)
    hot_rank = jax.random.permutation(key_hot, EXPERTS)
    is_hot = (hot_rank < hot_count).astype(jnp.int32)
    cell_ids = jnp.arange(cell_count, dtype=jnp.int32)
    noise_bits = jax.random.randint(key_score, (devices, cell_count), 0, 1 << 16)
    cell_score = is_hot[cell_ids // SLOTS][None, :] * (1 << 28) + noise_bits * cell_count + cell_ids[None, :]
    unused, chosen = lax.top_k(cell_score, T_DEV)
    device_ids = jnp.arange(devices, dtype=jnp.int32)[:, None]
    picked = jnp.zeros((devices, cell_count), jnp.int32).at[device_ids, chosen].set(1)
    slot_rank = jnp.cumsum(picked.reshape(devices, EXPERTS, SLOTS), axis=2).reshape(devices, cell_count) - 1
    chosen_rank = jnp.take_along_axis(slot_rank, chosen, axis=1)
    order_keys = jax.random.randint(key_order, (devices, T_DEV), 0, 1 << 16) * T_DEV + jnp.arange(T_DEV, dtype=jnp.int32)[None, :]
    token_order = jnp.argsort(order_keys, axis=1)
    token_cell = jnp.take_along_axis(chosen, token_order, axis=1)
    token_slots = jnp.take_along_axis(chosen_rank, token_order, axis=1)
    return ((token_cell // SLOTS).reshape(-1).astype(jnp.int32), token_slots.reshape(-1).astype(jnp.int32))


def draw_expert_id(key, part):
    return routing_pair(key)[0]


def draw_token_slot(key, part):
    return routing_pair(key)[1]


def draw_overflow_host(key, part):
    side_bits = jax.random.randint(jax.random.fold_in(key, 23), (EXPERTS, SPILL), 0, 2)
    expert_ids = jnp.arange(EXPERTS, dtype=jnp.int32)[:, None]
    return ((expert_ids + 2 * side_bits - 1 + EXPERTS) % EXPERTS).astype(jnp.int32)


def with_ends(values, stream_key, least, largest):
    longest = values.shape.index(max(values.shape))
    spots = []
    for shift in (0, 1):
        where = [jax.random.randint(jax.random.fold_in(stream_key, axis), (), 0, length) for axis, length in enumerate(values.shape)]
        where[longest] = (where[longest] + shift) % values.shape[longest]
        spots.append(tuple(where))
    return values.at[spots[0]].set(least).at[spots[1]].set(largest)


def level_of(own_key, dims, shards, least, top_value):
    gain, own = 1.0, jax.random.fold_in(own_key, 6)
    for dim, parts in shards:
        draws = jnp.exp(jax.random.uniform(jax.random.fold_in(own, dim), (parts,), jnp.float32, least / len(shards), top_value / len(shards)))
        gain = gain * jnp.repeat(draws, dims[dim] // parts).reshape([-1 if axis == dim else 1 for axis in range(len(dims))])
    return gain


def normal_values(own_key, shape, width, reach, shards=(), kind=jnp.bfloat16):
    gain = level_of(own_key, shape, shards, -0.22, 0.18) if shards else 1.0
    entries = jax.random.normal(own_key, shape, jnp.float32) * width * gain
    return jnp.minimum(jnp.maximum(entries, -reach), reach).astype(kind)


def setup_inputs(seed: int = 0, part: int = 0) -> dict:
    key_list = jax.random.split(jax.random.key(seed), 13)
    part_splits = jax.random.split(jax.random.fold_in(key_list[12], part), 13)
    return {
        "tokens": draw_tokens(jax.random.fold_in(jax.random.fold_in(key_list[12], part), 71), part),
        "router_logit": jnp.clip(3.0 * jax.random.uniform(part_splits[1], (TOKENS,), jnp.float32) ** level_of(part_splits[1], (TOKENS,), ((0, 8),), -0.2, 0.2), 0.0, 3.0),
        "expert_id": draw_expert_id(jax.random.fold_in(jax.random.fold_in(key_list[12], part), 71), part),
        "token_slot": draw_token_slot(jax.random.fold_in(jax.random.fold_in(key_list[12], part), 71), part),
        "keep": with_ends((jax.random.randint(part_splits[4], (TOKENS,), 0, 8) < 7).astype(jnp.int32), jax.random.fold_in(part_splits[4], 1), 0, 1),
        "overflow_host": draw_overflow_host(jax.random.fold_in(key_list[12], 71), part),
        "expert_gate": normal_values(key_list[6], (EXPERTS, D, F), (D // 2) ** -0.5, 0.125, ((0, 8),)),
        "expert_up": normal_values(key_list[7], (EXPERTS, D, F), (D // 2) ** -0.5, 0.125, ((0, 8),)),
        "expert_down": normal_values(key_list[8], (EXPERTS, F, D), F ** -0.5, 0.375, ((0, 8),)),
        "shared_gate": normal_values(key_list[9], (D, SH), D ** -0.5, 0.078125),
        "shared_up": normal_values(key_list[10], (D, SH), D ** -0.5, 0.078125),
        "shared_down": normal_values(key_list[11], (SH, D), (16 * SH) ** -0.5, 0.1875),
    }


def reference(tokens, router_logit, expert_id, token_slot, keep, overflow_host, expert_gate, expert_up, expert_down, shared_gate, shared_up, shared_down):
    token_scale = jax.nn.sigmoid(router_logit) * keep.astype(jnp.float32)
    routed_in = (tokens.astype(jnp.float32) * token_scale[:, None]).astype(jnp.bfloat16)
    is_spill = token_slot >= HOME
    spill_level = jnp.maximum(token_slot - HOME, 0).astype(jnp.int32)
    host_expert = overflow_host[expert_id, spill_level].astype(jnp.int32)
    served = jnp.where(is_spill, host_expert, expert_id).astype(jnp.int32)
    lane_count = HOME + 2 * SPILL
    positions = jnp.arange(TOKENS, dtype=jnp.int32)
    source_device = positions // T_DEV
    to_right = host_expert == (expert_id + 1) % EXPERTS
    lane_index = jnp.where(is_spill, jnp.where(to_right, HOME + spill_level, HOME + SPILL + spill_level), token_slot)
    column_index = (source_device * lane_count + lane_index).astype(jnp.int32)
    token_table = jnp.full((EXPERTS, EXPERTS * lane_count), TOKENS, jnp.int32).at[served, column_index].set(positions)
    padded = jnp.concatenate([routed_in, jnp.zeros((1, D), jnp.bfloat16)], axis=0)

    def one_expert(partial_value, inputs):
        index_row, w_gate, w_up, w_down = inputs
        chosen = padded[index_row]
        gate_out = jnp.dot(chosen, w_gate, preferred_element_type=jnp.float32)
        up_out = jnp.dot(chosen, w_up, preferred_element_type=jnp.float32)
        hidden = (jax.nn.silu(gate_out) * up_out).astype(jnp.bfloat16)
        result = jnp.dot(hidden, w_down, preferred_element_type=jnp.float32).astype(jnp.bfloat16)
        return partial_value.at[index_row].set(result), None

    routed, unused = lax.scan(one_expert, jnp.zeros((TOKENS + 1, D), jnp.bfloat16), (token_table, expert_gate, expert_up, expert_down))
    shared_hidden = (jax.nn.silu(jnp.dot(tokens, shared_gate, preferred_element_type=jnp.float32)) * jnp.dot(tokens, shared_up, preferred_element_type=jnp.float32)).astype(jnp.bfloat16)
    shared_out = jnp.dot(shared_hidden, shared_down, preferred_element_type=jnp.float32)
    return (shared_out + routed[:TOKENS].astype(jnp.float32)).astype(jnp.bfloat16)
```

```python
import functools

import jax
import jax.numpy as jnp
from jax import lax
from jax.experimental import pallas as pl
from jax.experimental.pallas import tpu as pltpu
from jax.sharding import PartitionSpec as P

MESH = pl.DeviceIdType.MESH


def expert_ffn(inputs, w_gate, w_up, w_down):
    flat_rows = inputs.reshape(-1, inputs.shape[-1])
    gate_out = jnp.dot(flat_rows, w_gate, preferred_element_type=jnp.float32)
    up_out = jnp.dot(flat_rows, w_up, preferred_element_type=jnp.float32)
    hidden = (jax.nn.silu(gate_out) * up_out).astype(jnp.bfloat16)
    result = jnp.dot(hidden, w_down, preferred_element_type=jnp.float32).astype(jnp.bfloat16)
    return result.reshape(inputs.shape)


def flip(index, step, count):
    out, bit = 0, 1
    while bit < count:
        out = out + bit * lax.rem(index // bit + step // bit, 2)
        bit *= 2
    return out


def moe_kernel(
    dps,
    experts,
    groups,
    home_pick,
    pool_pick,
    side_out,
    need_ref,
    scale_ref,
    tok_ref,
    wg_hbm,
    wu_hbm,
    wd_hbm,
    sg_ref,
    su_ref,
    home_ret,
    pool_ret,
    shared_ref,
    need_max,
    need_all,
    routed_in,
    home_out,
    pool_out,
    home_in,
    home_res,
    pool_in,
    pool_res,
    pool_part,
    pool_comb,
    side_in,
    wg,
    wu,
    wd,
    w_sem,
    own_sem,
    ns_sem,
    nr_sem,
    hs_sem,
    hr_sem,
    rs_sem,
    rr_sem,
    zs_sem,
    zr_sem,
    ms_sem,
    mr_sem,
    xs_sem,
    xr_sem,
    ps_sem,
    pr_sem,
    cs_sem,
    cr_sem,
):
    my_dp = lax.axis_index("dp")
    e = lax.axis_index("expert")
    g = e // 2
    p = e - 2 * g
    partner = e + 1 - 2 * p
    total = dps * experts
    me = my_dp * experts + e

    barrier = pltpu.get_barrier_semaphore()

    @pl.loop(1, total)
    def _(k):
        there = lax.rem(me + k, total)
        pl.semaphore_signal(
            barrier,
            inc=1,
            device_id={"dp": there // experts, "expert": lax.rem(there, experts)},
            device_id_type=MESH,
        )

    weights = [
        pltpu.make_async_copy(a, b, w_sem.at[i])
        for i, (a, b) in enumerate(((wg_hbm, wg), (wu_hbm, wu), (wd_hbm, wd)))
    ]
    own = [
        pltpu.make_async_copy(home_out.at[e], home_in.at[e], own_sem.at[0]),
        pltpu.make_async_copy(pool_out.at[g], pool_in.at[0, g], own_sem.at[1]),
        pltpu.make_async_copy(side_out.at[g], side_in.at[g], own_sem.at[2]),
        pltpu.make_async_copy(need_ref, need_all.at[me], own_sem.at[3]),
    ]

    def remote(src, dst, send, recv, to):
        return pltpu.make_async_remote_copy(
            src_ref=src,
            dst_ref=dst,
            send_sem=send,
            recv_sem=recv,
            device_id={"expert": to},
            device_id_type=MESH,
        )

    def n_copy(k):
        there = lax.rem(me + k, total)
        return pltpu.make_async_remote_copy(
            src_ref=need_ref,
            dst_ref=need_all.at[me],
            send_sem=ns_sem.at[k],
            recv_sem=nr_sem.at[k],
            device_id={"dp": there // experts, "expert": lax.rem(there, experts)},
            device_id_type=MESH,
        )

    def z_copy(k):
        to = flip(g, k, groups)
        return remote(pool_out.at[to], pool_in.at[0, g], zs_sem.at[k], zr_sem.at[k], 2 * to + p)

    def m_copy(k):
        to = flip(g, k, groups)
        return remote(side_out.at[to], side_in.at[g], ms_sem.at[k], mr_sem.at[k], 2 * to + p)

    def h_copy(k):
        to = flip(e, k, experts)
        return remote(home_out.at[to], home_in.at[e], hs_sem.at[k], hr_sem.at[k], to)

    def x_copy(k):
        origin = flip(g, k, groups)
        return remote(
            pool_in.at[0, origin],
            pool_in.at[1, flip(g, k, groups)],
            xs_sem.at[k],
            xr_sem.at[k],
            partner,
        )

    def p_copy(k):
        origin = flip(g, k, groups)
        return remote(
            pool_res.at[origin], pool_part.at[origin], ps_sem.at[k], pr_sem.at[k], partner
        )

    def c_copy(k):
        origin = flip(g, k, groups)
        return remote(
            pool_comb.at[origin], pool_ret.at[g], cs_sem.at[k], cr_sem.at[k], 2 * origin + p
        )

    def r_copy(k):
        origin = flip(e, k, experts)
        return remote(home_res.at[origin], home_ret.at[e], rs_sem.at[k], rr_sem.at[k], origin)

    def rows_of(pick):
        return jnp.dot(pick, routed_in[...], preferred_element_type=jnp.float32).astype(jnp.bfloat16)

    routed_in[...] = (tok_ref[...].astype(jnp.float32) * scale_ref[...]).astype(jnp.bfloat16)

    pl.semaphore_wait(barrier, total - 1)

    @pl.loop(1, groups + 1)
    def _(i):
        k = groups - i
        to = flip(g, k, groups)
        pool_out[to] = rows_of(pool_pick[to])

        @pl.when(i > 1)
        def _():
            z_copy(k + 1).start()
            m_copy(k + 1).start()

    @pl.loop(1, experts + 1)
    def _(i):
        k = experts - i
        to = flip(e, k, experts)
        home_out[to] = rows_of(home_pick[to])

        @pl.when(i > 1)
        def _():
            h_copy(k + 1).start()

    for copy in own:
        copy.start()
    for copy in weights:
        copy.start()

    @pl.loop(1, total)
    def _(k):
        n_copy(k).start()

    for copy in own:
        copy.wait()
    x_copy(0).start()

    tok = tok_ref[...]
    last = (((1,), (1,)), ((), ()))
    shared_gate = lax.dot_general(tok, sg_ref[...], last, preferred_element_type=jnp.float32)
    shared_up = lax.dot_general(tok, su_ref[...], last, preferred_element_type=jnp.float32)
    shared_ref[...] = (jax.nn.silu(shared_gate) * shared_up).astype(jnp.bfloat16)

    for copy in weights:
        copy.wait()

    def ffn(x):
        gate_out = jnp.dot(x, wg[...], preferred_element_type=jnp.float32)
        up_out = jnp.dot(x, wu[...], preferred_element_type=jnp.float32)
        hidden = (jax.nn.silu(gate_out) * up_out).astype(jnp.bfloat16)
        return jnp.dot(hidden, wd[...], preferred_element_type=jnp.float32).astype(jnp.bfloat16)

    home_res[e] = ffn(home_in[e])
    own_ret = pltpu.make_async_copy(home_res.at[e], home_ret.at[e], own_sem.at[0])
    own_ret.start()

    @pl.loop(1, groups)
    def _(i):
        k = groups - i
        z_copy(k).wait_recv()
        x_copy(k).start()

    def home_block(i):
        k = experts - i
        origin = flip(e, k, experts)
        h_copy(k).wait_recv()
        home_res[origin] = ffn(home_in[origin])
        r_copy(k).start()

    @pl.loop(1, groups + 1)
    def _(i):
        k = groups - i
        origin = flip(g, k, groups)
        x_copy(k).wait_recv()
        pool_res[origin] = ffn(pool_in[1, origin])
        p_copy(k).start()

    @pl.loop(1, groups + 1)
    def _(i):
        k = groups - i
        origin = flip(g, k, groups)
        mine = ffn(pool_in[0, origin])
        p_copy(k).wait_recv()

        @pl.when(k > 0)
        def _():
            m_copy(k).wait_recv()

        here = jnp.abs(side_in[origin][:, :1] - p.astype(jnp.float32)) < 0.5
        pool_comb[origin] = jnp.where(here, mine, pool_part[origin])

        @pl.when(k > 0)
        def _():
            c_copy(k).start()

    own_back = pltpu.make_async_copy(pool_comb.at[g], pool_ret.at[g], own_sem.at[1])
    own_back.start()

    pl.loop(1, experts)(home_block)

    @pl.loop(0, groups)
    def _(k):
        x_copy(k).wait_send()
        p_copy(k).wait_send()

    @pl.loop(1, groups)
    def _(k):
        z_copy(k).wait_send()
        m_copy(k).wait_send()
        c_copy(k).wait()

    @pl.loop(1, total)
    def _(k):
        n_copy(k).wait()

    @pl.loop(1, experts)
    def _(k):
        h_copy(k).wait_send()
        r_copy(k).wait()

    own_ret.wait()
    own_back.wait()
    need_max[...] = jnp.max(need_all[...], axis=0)


def routed_exchange(
    home_pick, pool_pick, side_out, need, scale, tokens, w_gate, w_up, w_down, shared_gate, shared_up
):
    dps, experts = lax.axis_size("dp"), lax.axis_size("expert")
    groups = pool_pick.shape[0]
    width = tokens.shape[1]
    home_shape, pool_shape = home_pick.shape[:2] + (width,), pool_pick.shape[:2] + (width,)
    bf16 = jnp.bfloat16
    vmem = pl.BlockSpec(memory_space=pltpu.VMEM)
    anywhere = pl.BlockSpec(memory_space=pl.ANY)
    dma = pltpu.SemaphoreType.DMA
    return pl.pallas_call(
        functools.partial(moe_kernel, dps, experts, groups),
        out_shape=(
            jax.ShapeDtypeStruct(home_shape, bf16),
            jax.ShapeDtypeStruct(pool_shape, bf16),
            jax.ShapeDtypeStruct((tokens.shape[0], shared_gate.shape[0]), bf16),
            jax.ShapeDtypeStruct(need.shape, need.dtype),
        ),
        in_specs=[vmem] * 6 + [anywhere] * 3 + [vmem] * 2,
        out_specs=(vmem,) * 4,
        scratch_shapes=[
            pltpu.VMEM((dps * experts,) + need.shape, need.dtype),
            pltpu.VMEM(tokens.shape, bf16),
            pltpu.VMEM(home_shape, bf16),
            pltpu.VMEM(pool_shape, bf16),
            pltpu.VMEM(home_shape, bf16),
            pltpu.VMEM(home_shape, bf16),
            pltpu.VMEM((2,) + pool_shape, bf16),
            pltpu.VMEM(pool_shape, bf16),
            pltpu.VMEM(pool_shape, bf16),
            pltpu.VMEM(pool_shape, bf16),
            pltpu.VMEM(side_out.shape, jnp.float32),
            pltpu.VMEM(w_gate.shape, bf16),
            pltpu.VMEM(w_up.shape, bf16),
            pltpu.VMEM(w_down.shape, bf16),
            dma((3,)),
            dma((4,)),
        ]
        + [dma((dps * experts,))] * 2
        + [dma((experts,))] * 4
        + [dma((groups,))] * 10,
        compiler_params=pltpu.CompilerParams(
            collective_id=0, has_side_effects=True, vmem_limit_bytes=60 * 1024 * 1024
        ),
        name="moe",
    )(home_pick, pool_pick, side_out, need, scale, tokens, w_gate, w_up, w_down, shared_gate, shared_up)


def split_columns(total, step=256):
    out, at = [], 0
    while at < total:
        out.append((at, min(step, total - at)))
        at += step
    return out


def slab_kernel(
    dps,
    experts,
    groups,
    need_ref,
    home_pick,
    pool_pick,
    back_ref,
    sel_ref,
    scale_ref,
    tok_ref,
    wg_hbm,
    wu_hbm,
    wd_hbm,
    sg_ref,
    su_ref,
    out_ref,
    shared_ref,
    need_max,
    need_all,
    routed_in,
    home_out,
    pool_out,
    home_in,
    pool_in,
    res,
    ret,
    wg,
    wu,
    slab,
    sel_all,
    h_all,
    spread,
    stage,
    w_sem,
    own_sem,
    ns_sem,
    nr_sem,
    hs_sem,
    hr_sem,
    rs_sem,
    rr_sem,
    zs_sem,
    zr_sem,
    xs_sem,
    xr_sem,
    ls_sem,
    lr_sem,
    gs_sem,
    gr_sem,
    os_sem,
    or_sem,
    vs_sem,
    vr_sem,
    ss_sem,
    sr_sem,
):
    my_dp = lax.axis_index("dp")
    e = lax.axis_index("expert")
    g = e // 2
    p = e - 2 * g
    partner = e + 1 - 2 * p
    total = dps * experts
    me = my_dp * experts + e
    members = 2 * dps
    j = p * dps + my_dp
    half = groups // 2
    mate = flip(g, 1, groups)
    far_mid = jnp.where(g < half, half, half - 1)
    far_end = flip(far_mid, 1, groups)
    is_mid = (g == half) | (g == half - 1)
    direct = home_pick.shape[1]
    pooled = pool_pick.shape[1]
    rows, width = tok_ref.shape
    hid = wg.shape[1]
    ncols = slab.shape[3]
    chunks = split_columns(ncols)

    barrier = pltpu.get_barrier_semaphore()

    @pl.loop(1, total)
    def _(k):
        there = lax.rem(me + k, total)
        pl.semaphore_signal(
            barrier,
            inc=1,
            device_id={"dp": there // experts, "expert": lax.rem(there, experts)},
            device_id_type=MESH,
        )

    def columns(member, at=0, count=ncols):
        return pl.ds(pl.multiple_of(member * ncols + at, 128), count)

    weights = [
        pltpu.make_async_copy(a, b, w_sem.at[i])
        for i, (a, b) in enumerate(((wg_hbm, wg), (wu_hbm, wu)))
    ]
    own_slab = pltpu.make_async_copy(wd_hbm.at[:, columns(j)], slab.at[g, p], w_sem.at[2])
    own = [
        pltpu.make_async_copy(home_out.at[e], home_in.at[e], own_sem.at[0]),
        pltpu.make_async_copy(pool_out.at[g], pool_in.at[g, 0], own_sem.at[1]),
        pltpu.make_async_copy(need_ref, need_all.at[me], own_sem.at[2]),
        pltpu.make_async_copy(sel_ref, sel_all.at[j], own_sem.at[3]),
    ]

    def remote(src, dst, send, recv, to):
        return pltpu.make_async_remote_copy(
            src_ref=src,
            dst_ref=dst,
            send_sem=send,
            recv_sem=recv,
            device_id=to,
            device_id_type=MESH,
        )

    def n_copy(k):
        there = lax.rem(me + k, total)
        to = {"dp": there // experts, "expert": lax.rem(there, experts)}
        return remote(need_ref, need_all.at[me], ns_sem.at[k], nr_sem.at[k], to)

    def z_copy(k):
        to = flip(g, k, groups)
        there = {"expert": 2 * to + p}
        return remote(pool_out.at[to], pool_in.at[g, 0], zs_sem.at[k], zr_sem.at[k], there)

    def h_copy(k):
        to = flip(e, k, experts)
        return remote(home_out.at[to], home_in.at[e], hs_sem.at[k], hr_sem.at[k], {"expert": to})

    def x_copy(k):
        origin = flip(g, k, groups)
        return remote(
            pool_in.at[origin, 0],
            pool_in.at[flip(g, k, groups), 1],
            xs_sem.at[k],
            xr_sem.at[k],
            {"expert": partner},
        )

    def r_copy(k):
        origin = flip(e, k, experts)
        return remote(res.at[origin], ret.at[e], rs_sem.at[k], rr_sem.at[k], {"expert": origin})

    def peer(k):
        m = flip(j, k, members)
        return m, {"dp": lax.rem(m, dps), "expert": 2 * g + m // dps}

    def l_copy(k):
        return remote(sel_ref, sel_all.at[j], ls_sem.at[k], lr_sem.at[k], peer(k)[1])

    def g_copy(k):
        return remote(h_all.at[j], h_all.at[j], gs_sem.at[k], gr_sem.at[k], peer(k)[1])

    def o_copy(k, c):
        at, count = chunks[c]
        m, there = peer(k)
        return remote(
            stage.at[m, :, pl.ds(at, count)],
            out_ref.at[:, columns(j, at, count)],
            os_sem.at[k, c],
            or_sem.at[k, c],
            there,
        )

    def v_copy():
        j_there = (1 - p) * dps + my_dp
        return remote(
            wd_hbm.at[:, columns(j_there)],
            slab.at[g, p],
            vs_sem.at[0],
            vr_sem.at[0],
            {"expert": partner},
        )

    def s_copy(block, c, slot, to):
        at, count = chunks[c]
        part = slab.at[block, :, :, pl.ds(at, count)]
        return remote(part, part, ss_sem.at[slot, c], sr_sem.at[block, c], {"expert": 2 * to + p})

    def rows_of(pick):
        return jnp.dot(pick, routed_in[...], preferred_element_type=jnp.float32).astype(jnp.bfloat16)

    for copy in weights:
        copy.start()
    own_slab.start()
    routed_in[...] = (tok_ref[...].astype(jnp.float32) * scale_ref[...]).astype(jnp.bfloat16)
    res[...] = jnp.zeros_like(res)

    pl.semaphore_wait(barrier, total - 1)

    @pl.loop(1, groups + 1)
    def _(i):
        k = groups - i
        to = flip(g, k, groups)
        pool_out[to] = rows_of(pool_pick[to])

        @pl.when(i > 1)
        def _():
            z_copy(k + 1).start()

    @pl.loop(1, experts + 1)
    def _(i):
        k = experts - i
        to = flip(e, k, experts)
        home_out[to] = rows_of(home_pick[to])

        @pl.when(i > 1)
        def _():
            h_copy(k + 1).start()

    for copy in own:
        copy.start()
    v_copy().start()

    @pl.loop(1, total)
    def _(k):
        n_copy(k).start()

    @pl.loop(1, members)
    def _(k):
        l_copy(k).start()

    for copy in own:
        copy.wait()
    x_copy(0).start()

    tok = tok_ref[...]
    last = (((1,), (1,)), ((), ()))
    shared_gate = lax.dot_general(tok, sg_ref[...], last, preferred_element_type=jnp.float32)
    shared_up = lax.dot_general(tok, su_ref[...], last, preferred_element_type=jnp.float32)
    shared_ref[...] = (jax.nn.silu(shared_gate) * shared_up).astype(jnp.bfloat16)

    own_slab.wait()
    v_copy().wait_recv()
    for c in range(len(chunks)):
        s_copy(g, c, 1, far_mid).start()
        s_copy(g, c, 0, mate).start()

    for copy in weights:
        copy.wait()

    def hidden_of(x):
        gate_out = jnp.dot(x, wg[...], preferred_element_type=jnp.float32)
        up_out = jnp.dot(x, wu[...], preferred_element_type=jnp.float32)
        return (jax.nn.silu(gate_out) * up_out).astype(jnp.bfloat16)

    res[e, :direct, :] = hidden_of(home_in[e])

    @pl.loop(1, groups)
    def _(i):
        k = groups - i
        z_copy(k).wait_recv()
        x_copy(k).start()

    base = (direct + 15) // 16 * 16

    @pl.loop(1, groups + 1)
    def _(i):
        k = groups - i
        origin = flip(g, k, groups)
        x_copy(k).wait_recv()
        both = hidden_of(pool_in[origin].reshape(2 * pooled, width))
        res[2 * origin + p, base : base + pooled, :] = both[:pooled]
        res[2 * origin + 1 - p, base : base + pooled, :] = both[pooled:]

    own_ret = pltpu.make_async_copy(res.at[e], ret.at[e], own_sem.at[0])
    own_ret.start()

    @pl.loop(1, experts)
    def _(i):
        k = experts - i
        origin = flip(e, k, experts)
        h_copy(k).wait_recv()
        res[origin, :direct, :] = hidden_of(home_in[origin])
        r_copy(k).start()

    own_ret.wait()

    @pl.loop(1, experts)
    def _(i):
        r_copy(experts - i).wait_recv()

    found = jnp.dot(
        back_ref[...], ret[...].reshape(-1, hid), preferred_element_type=jnp.float32
    )
    h_all[j] = found.astype(jnp.bfloat16)

    @pl.loop(1, members)
    def _(i):
        g_copy(members - i).start()

    def expand(m):
        values = h_all[m]
        marks = sel_all[m].astype(jnp.float32)
        for x in range(experts):
            mark = marks[:, x : x + 1] > 0.5
            spread[m, :, x * hid : (x + 1) * hid] = jnp.where(mark, values, jnp.zeros_like(values))

    def slab_arrive(c):
        @pl.when(is_mid)
        def _():
            for slot, block in ((2, far_mid), (3, far_end)):
                s_copy(block, c, slot, mate).wait_recv()
                s_copy(block, c, slot, mate).start()

        s_copy(mate, c, 0, mate).wait_recv()

        @pl.when(jnp.logical_not(is_mid))
        def _():
            for block in (far_mid, far_end):
                s_copy(block, c, 2, mate).wait_recv()

    def project(m, c):
        at, count = chunks[c]
        w = slab[:, :, :, at : at + count].reshape(experts * hid, count)
        y = jnp.dot(spread[m], w, preferred_element_type=jnp.float32)
        stage[m, :, at : at + count] = y.astype(jnp.bfloat16)

    expand(j)
    slab_arrive(0)

    @pl.loop(1, members)
    def _(i):
        k = members - i
        l_copy(k).wait_recv()
        g_copy(k).wait_recv()
        expand(peer(k)[0])

    def own_out(c):
        at, count = chunks[c]
        return pltpu.make_async_copy(
            stage.at[j, :, pl.ds(at, count)],
            out_ref.at[:, columns(j, at, count)],
            os_sem.at[0, c],
        )

    for c in range(len(chunks)):
        if c + 1 < len(chunks):
            slab_arrive(c + 1)

        @pl.loop(1, members)
        def _(i):
            k = members - i
            project(peer(k)[0], c)
            o_copy(k, c).start()

        project(j, c)
        own_out(c).start()

    for c in range(len(chunks)):

        @pl.loop(1, members)
        def _(k):
            o_copy(k, c).wait()

        own_out(c).wait()
        s_copy(g, c, 1, far_mid).wait_send()
        s_copy(g, c, 0, mate).wait_send()

        @pl.when(is_mid)
        def _():
            for slot, block in ((2, far_mid), (3, far_end)):
                s_copy(block, c, slot, mate).wait_send()

    v_copy().wait_send()

    @pl.loop(0, groups)
    def _(k):
        x_copy(k).wait_send()

    @pl.loop(1, groups)
    def _(k):
        z_copy(k).wait_send()

    @pl.loop(1, total)
    def _(k):
        n_copy(k).wait()

    @pl.loop(1, members)
    def _(k):
        l_copy(k).wait_send()
        g_copy(k).wait_send()

    @pl.loop(1, experts)
    def _(k):
        h_copy(k).wait_send()
        r_copy(k).wait_send()

    need_max[...] = jnp.max(need_all[...], axis=0)


def slab_exchange(
    need, home_pick, pool_pick, back, sel, scale, tokens, w_gate, w_up, w_down, shared_gate, shared_up
):
    dps, experts = lax.axis_size("dp"), lax.axis_size("expert")
    groups = pool_pick.shape[0]
    rows, width = tokens.shape
    hid = w_gate.shape[1]
    members = 2 * dps
    ncols = width // members
    parts = len(split_columns(ncols))
    direct, pooled = home_pick.shape[1], pool_pick.shape[1]
    cell = (direct + 15) // 16 * 16 + pooled
    bf16 = jnp.bfloat16
    vmem = pl.BlockSpec(memory_space=pltpu.VMEM)
    anywhere = pl.BlockSpec(memory_space=pl.ANY)
    dma = pltpu.SemaphoreType.DMA
    return pl.pallas_call(
        functools.partial(slab_kernel, dps, experts, groups),
        out_shape=(
            jax.ShapeDtypeStruct((rows, width), bf16),
            jax.ShapeDtypeStruct((rows, shared_gate.shape[0]), bf16),
            jax.ShapeDtypeStruct(need.shape, need.dtype),
        ),
        in_specs=[vmem] * 7 + [anywhere] * 3 + [vmem] * 2,
        out_specs=(vmem,) * 3,
        scratch_shapes=[
            pltpu.VMEM((dps * experts,) + need.shape, need.dtype),
            pltpu.VMEM((rows, width), bf16),
            pltpu.VMEM((experts, direct, width), bf16),
            pltpu.VMEM((groups, pooled, width), bf16),
            pltpu.VMEM((experts, direct, width), bf16),
            pltpu.VMEM((groups, 2, pooled, width), bf16),
            pltpu.VMEM((experts, cell, hid), bf16),
            pltpu.VMEM((experts, cell, hid), bf16),
            pltpu.VMEM(w_gate.shape, bf16),
            pltpu.VMEM(w_up.shape, bf16),
            pltpu.VMEM((groups, 2, hid, ncols), bf16),
            pltpu.VMEM((members,) + sel.shape, bf16),
            pltpu.VMEM((members, rows, hid), bf16),
            pltpu.VMEM((members, rows, experts * hid), bf16),
            pltpu.VMEM((members, rows, ncols), bf16),
            dma((3,)),
            dma((4,)),
        ]
        + [dma((dps * experts,))] * 2
        + [dma((experts,))] * 4
        + [dma((groups,))] * 4
        + [dma((members,))] * 4
        + [dma((members, parts))] * 2
        + [dma((1,))] * 2
        + [dma((4, parts)), dma((groups, parts))],
        compiler_params=pltpu.CompilerParams(
            collective_id=1, has_side_effects=True, vmem_limit_bytes=60 * 1024 * 1024
        ),
        name="slab_moe",
    )(need, home_pick, pool_pick, back, sel, scale, tokens, w_gate, w_up, w_down, shared_gate, shared_up)


def body(
    tokens,
    router_logit,
    expert_id,
    token_slot,
    keep,
    overflow_host,
    expert_gate,
    expert_up,
    expert_down,
    shared_gate,
    shared_up,
    shared_down,
):
    experts = lax.axis_size("expert")
    dps = lax.axis_size("dp")
    groups = experts // 2
    my_e = lax.axis_index("expert")
    tok_count, model_width = tokens.shape
    slot_count = 2 * tok_count // experts
    home_count = slot_count // 2
    spill_count = slot_count - home_count
    w_gate, w_up, w_down = expert_gate[0], expert_up[0], expert_down[0]
    token_scale = jax.nn.sigmoid(router_logit) * keep.astype(jnp.float32)
    positions = jnp.arange(tok_count, dtype=jnp.int32)
    is_spill = token_slot >= home_count
    spill_level = jnp.maximum(token_slot - home_count, 0)
    table_index = expert_id * spill_count + spill_level
    table_ids = jnp.arange(experts * spill_count, dtype=jnp.int32)
    host_expert = jnp.sum(
        jnp.where(table_index[:, None] == table_ids[None, :], overflow_host.reshape(1, -1), 0),
        axis=1,
    )
    served = jnp.where(is_spill, host_expert, expert_id)
    kept = keep != 0
    before = positions[None, :] < positions[:, None]

    def rank_of(member, label):
        same = (label[:, None] == label[None, :]) & member[None, :] & before
        return jnp.sum(same.astype(jnp.int32), axis=1)

    direct = max(1, 3 * home_count // 4)
    pooled = home_count
    direct_rank = rank_of(kept, served)
    over = kept & (direct_rank >= direct)
    pool_rank = rank_of(over, served // 2)
    left = over & (pool_rank >= pooled)
    home_cell = jnp.where(kept & ~over, served * direct + direct_rank, -1)
    pool_cell = jnp.where(over & ~left, (served // 2) * pooled + pool_rank, -1)
    home_ids = jnp.arange(experts * direct, dtype=jnp.int32)
    pool_ids = jnp.arange(groups * pooled, dtype=jnp.int32)
    home_pick = (home_ids[:, None] == home_cell[None, :]).astype(jnp.bfloat16)
    pool_pick = (pool_ids[:, None] == pool_cell[None, :]).astype(jnp.bfloat16)
    unserved = jnp.broadcast_to(jnp.max(left.astype(jnp.int32)), (8, 128))
    if groups == 4 and model_width % (2 * dps * 128) == 0:
        cell = (direct + 15) // 16 * 16
        spot = jnp.where(over, cell + pool_rank, direct_rank)
        stride = cell + pooled
        back_cell = jnp.where(kept & ~left, served * stride + spot, -1)
        back_ids = jnp.arange(experts * stride, dtype=jnp.int32)
        back = (back_cell[:, None] == back_ids[None, :]).astype(jnp.bfloat16)
        expert_ids = jnp.arange(128, dtype=jnp.int32)
        sel = (jnp.where(kept & ~left, served, -1)[:, None] == expert_ids[None, :]).astype(
            jnp.bfloat16
        )
        routed, shared_hidden, unserved_all = slab_exchange(
            unserved,
            home_pick.reshape(experts, direct, tok_count),
            pool_pick.reshape(groups, pooled, tok_count),
            back,
            sel,
            token_scale[:, None],
            tokens,
            w_gate,
            w_up,
            w_down,
            shared_gate.T,
            shared_up.T,
        )

        def combined():
            shared = jnp.dot(shared_hidden, shared_down, preferred_element_type=jnp.float32)
            return shared + routed.astype(jnp.float32)

    else:
        side = jnp.sum(
            jnp.where(pool_ids[:, None] == pool_cell[None, :], (served % 2)[None, :], 0), axis=1
        )
        side_out = jnp.broadcast_to(side.astype(jnp.float32)[:, None], (groups * pooled, 128))
        home_ret, pool_ret, shared_hidden, unserved_all = routed_exchange(
            home_pick.reshape(experts, direct, tok_count),
            pool_pick.reshape(groups, pooled, tok_count),
            side_out.reshape(groups, pooled, 128),
            unserved,
            token_scale[:, None],
            tokens,
            w_gate,
            w_up,
            w_down,
            shared_gate.T,
            shared_up.T,
        )

        def combined():
            home_back = (home_cell[:, None] == home_ids[None, :]).astype(jnp.bfloat16)
            pool_back = (pool_cell[:, None] == pool_ids[None, :]).astype(jnp.bfloat16)
            pick = jnp.concatenate([home_back, pool_back, shared_hidden], axis=1)
            source = jnp.concatenate(
                [home_ret.reshape(-1, model_width), pool_ret.reshape(-1, model_width), shared_down],
                axis=0,
            )
            return jnp.dot(pick, source, preferred_element_type=jnp.float32)

    def all_served():
        return combined().astype(jnp.bfloat16)

    def some_left():
        rows = (tokens.astype(jnp.float32) * token_scale[:, None]).astype(jnp.bfloat16)
        lanes = home_count + 2 * spill_count
        to_right = host_expert == (expert_id + 1) % experts
        lane_index = jnp.where(
            is_spill,
            home_count + spill_level + jnp.where(to_right, 0, spill_count),
            token_slot,
        )
        cell_index = served * lanes + lane_index
        source_row = jnp.zeros((experts * lanes,), jnp.int32).at[cell_index].set(positions)
        outgoing = rows[source_row].reshape(experts, lanes, model_width)
        incoming = lax.all_to_all(outgoing, "expert", split_axis=0, concat_axis=0, tiled=True)
        answers = lax.all_to_all(
            expert_ffn(incoming, w_gate, w_up, w_down),
            "expert",
            split_axis=0,
            concat_axis=0,
            tiled=True,
        )
        rest = answers.reshape(-1, model_width)[cell_index].astype(jnp.float32)
        return (combined() + jnp.where(left[:, None], rest, 0.0)).astype(jnp.bfloat16)

    return lax.cond(unserved_all[0, 0] > 0, some_left, all_served)


def solution(mesh):
    return jax.shard_map(
        body,
        mesh=mesh,
        in_specs=(
            P(("dp", "expert"), None),
            P(("dp", "expert")),
            P(("dp", "expert")),
            P(("dp", "expert")),
            P(("dp", "expert")),
            P(),
            P("expert", None, None),
            P("expert", None, None),
            P("expert", None, None),
            P(),
            P(),
            P(),
        ),
        out_specs=P(("dp", "expert"), None),
        check_vma=False,
    )
```

```python
import functools

import jax
import jax.numpy as jnp
from jax import lax
from jax.experimental import pallas as pl
from jax.experimental.pallas import tpu as pltpu
from jax.sharding import PartitionSpec as P

MESH = pl.DeviceIdType.MESH


def expert_ffn(inputs, w_gate, w_up, w_down):
    flat_rows = inputs.reshape(-1, inputs.shape[-1])
    gate_out = jnp.dot(flat_rows, w_gate, preferred_element_type=jnp.float32)
    up_out = jnp.dot(flat_rows, w_up, preferred_element_type=jnp.float32)
    hidden = (jax.nn.silu(gate_out) * up_out).astype(jnp.bfloat16)
    result = jnp.dot(hidden, w_down, preferred_element_type=jnp.float32).astype(jnp.bfloat16)
    return result.reshape(inputs.shape)


def flip(index, step, count):
    out, bit = 0, 1
    while bit < count:
        out = out + bit * lax.rem(index // bit + step // bit, 2)
        bit *= 2
    return out


def moe_kernel(
    dps,
    experts,
    groups,
    home_pick,
    pool_pick,
    side_out,
    need_ref,
    scale_ref,
    tok_ref,
    wg_hbm,
    wu_hbm,
    wd_hbm,
    sg_ref,
    su_ref,
    home_ret,
    pool_ret,
    shared_ref,
    need_max,
    need_all,
    routed_in,
    home_out,
    pool_out,
    home_in,
    home_res,
    pool_in,
    pool_res,
    pool_part,
    pool_comb,
    side_in,
    wg,
    wu,
    wd,
    w_sem,
    own_sem,
    ns_sem,
    nr_sem,
    hs_sem,
    hr_sem,
    rs_sem,
    rr_sem,
    zs_sem,
    zr_sem,
    ms_sem,
    mr_sem,
    xs_sem,
    xr_sem,
    ps_sem,
    pr_sem,
    cs_sem,
    cr_sem,
):
    my_dp = lax.axis_index("dp")
    e = lax.axis_index("expert")
    g = e // 2
    p = e - 2 * g
    partner = e + 1 - 2 * p
    total = dps * experts
    me = my_dp * experts + e

    barrier = pltpu.get_barrier_semaphore()

    @pl.loop(1, total)
    def _(k):
        there = lax.rem(me + k, total)
        pl.semaphore_signal(
            barrier,
            inc=1,
            device_id={"dp": there // experts, "expert": lax.rem(there, experts)},
            device_id_type=MESH,
        )

    weights = [
        pltpu.make_async_copy(a, b, w_sem.at[i])
        for i, (a, b) in enumerate(((wg_hbm, wg), (wu_hbm, wu), (wd_hbm, wd)))
    ]
    own = [
        pltpu.make_async_copy(home_out.at[e], home_in.at[e], own_sem.at[0]),
        pltpu.make_async_copy(pool_out.at[g], pool_in.at[0, g], own_sem.at[1]),
        pltpu.make_async_copy(side_out.at[g], side_in.at[g], own_sem.at[2]),
        pltpu.make_async_copy(need_ref, need_all.at[me], own_sem.at[3]),
    ]

    def remote(src, dst, send, recv, to):
        return pltpu.make_async_remote_copy(
            src_ref=src,
            dst_ref=dst,
            send_sem=send,
            recv_sem=recv,
            device_id={"expert": to},
            device_id_type=MESH,
        )

    def n_copy(k):
        there = lax.rem(me + k, total)
        return pltpu.make_async_remote_copy(
            src_ref=need_ref,
            dst_ref=need_all.at[me],
            send_sem=ns_sem.at[k],
            recv_sem=nr_sem.at[k],
            device_id={"dp": there // experts, "expert": lax.rem(there, experts)},
            device_id_type=MESH,
        )

    def z_copy(k):
        to = flip(g, k, groups)
        return remote(pool_out.at[to], pool_in.at[0, g], zs_sem.at[k], zr_sem.at[k], 2 * to + p)

    def m_copy(k):
        to = flip(g, k, groups)
        return remote(side_out.at[to], side_in.at[g], ms_sem.at[k], mr_sem.at[k], 2 * to + p)

    def h_copy(k):
        to = flip(e, k, experts)
        return remote(home_out.at[to], home_in.at[e], hs_sem.at[k], hr_sem.at[k], to)

    def x_copy(k):
        origin = flip(g, k, groups)
        return remote(
            pool_in.at[0, origin],
            pool_in.at[1, flip(g, k, groups)],
            xs_sem.at[k],
            xr_sem.at[k],
            partner,
        )

    def p_copy(k):
        origin = flip(g, k, groups)
        return remote(
            pool_res.at[origin], pool_part.at[origin], ps_sem.at[k], pr_sem.at[k], partner
        )

    def c_copy(k):
        origin = flip(g, k, groups)
        return remote(
            pool_comb.at[origin], pool_ret.at[g], cs_sem.at[k], cr_sem.at[k], 2 * origin + p
        )

    def r_copy(k):
        origin = flip(e, k, experts)
        return remote(home_res.at[origin], home_ret.at[e], rs_sem.at[k], rr_sem.at[k], origin)

    def rows_of(pick):
        return jnp.dot(pick, routed_in[...], preferred_element_type=jnp.float32).astype(jnp.bfloat16)

    routed_in[...] = (tok_ref[...].astype(jnp.float32) * scale_ref[...]).astype(jnp.bfloat16)

    pl.semaphore_wait(barrier, total - 1)

    @pl.loop(1, groups + 1)
    def _(i):
        k = groups - i
        to = flip(g, k, groups)
        pool_out[to] = rows_of(pool_pick[to])

        @pl.when(i > 1)
        def _():
            z_copy(k + 1).start()
            m_copy(k + 1).start()

    @pl.loop(1, experts + 1)
    def _(i):
        k = experts - i
        to = flip(e, k, experts)
        home_out[to] = rows_of(home_pick[to])

        @pl.when(i > 1)
        def _():
            h_copy(k + 1).start()

    for copy in own:
        copy.start()
    for copy in weights:
        copy.start()

    @pl.loop(1, total)
    def _(k):
        n_copy(k).start()

    for copy in own:
        copy.wait()
    x_copy(0).start()

    tok = tok_ref[...]
    last = (((1,), (1,)), ((), ()))
    shared_gate = lax.dot_general(tok, sg_ref[...], last, preferred_element_type=jnp.float32)
    shared_up = lax.dot_general(tok, su_ref[...], last, preferred_element_type=jnp.float32)
    shared_ref[...] = (jax.nn.silu(shared_gate) * shared_up).astype(jnp.bfloat16)

    for copy in weights:
        copy.wait()

    def ffn(x):
        gate_out = jnp.dot(x, wg[...], preferred_element_type=jnp.float32)
        up_out = jnp.dot(x, wu[...], preferred_element_type=jnp.float32)
        hidden = (jax.nn.silu(gate_out) * up_out).astype(jnp.bfloat16)
        return jnp.dot(hidden, wd[...], preferred_element_type=jnp.float32).astype(jnp.bfloat16)

    home_res[e] = ffn(home_in[e])
    own_ret = pltpu.make_async_copy(home_res.at[e], home_ret.at[e], own_sem.at[0])
    own_ret.start()

    @pl.loop(1, groups)
    def _(i):
        k = groups - i
        z_copy(k).wait_recv()
        x_copy(k).start()

    def home_block(i):
        k = experts - i
        origin = flip(e, k, experts)
        h_copy(k).wait_recv()
        home_res[origin] = ffn(home_in[origin])
        r_copy(k).start()

    @pl.loop(1, groups + 1)
    def _(i):
        k = groups - i
        origin = flip(g, k, groups)
        x_copy(k).wait_recv()
        pool_res[origin] = ffn(pool_in[1, origin])
        p_copy(k).start()

    @pl.loop(1, groups + 1)
    def _(i):
        k = groups - i
        origin = flip(g, k, groups)
        mine = ffn(pool_in[0, origin])
        p_copy(k).wait_recv()

        @pl.when(k > 0)
        def _():
            m_copy(k).wait_recv()

        here = jnp.abs(side_in[origin][:, :1] - p.astype(jnp.float32)) < 0.5
        pool_comb[origin] = jnp.where(here, mine, pool_part[origin])

        @pl.when(k > 0)
        def _():
            c_copy(k).start()

    own_back = pltpu.make_async_copy(pool_comb.at[g], pool_ret.at[g], own_sem.at[1])
    own_back.start()

    pl.loop(1, experts)(home_block)

    @pl.loop(0, groups)
    def _(k):
        x_copy(k).wait_send()
        p_copy(k).wait_send()

    @pl.loop(1, groups)
    def _(k):
        z_copy(k).wait_send()
        m_copy(k).wait_send()
        c_copy(k).wait()

    @pl.loop(1, total)
    def _(k):
        n_copy(k).wait()

    @pl.loop(1, experts)
    def _(k):
        h_copy(k).wait_send()
        r_copy(k).wait()

    own_ret.wait()
    own_back.wait()
    need_max[...] = jnp.max(need_all[...], axis=0)


def routed_exchange(
    home_pick, pool_pick, side_out, need, scale, tokens, w_gate, w_up, w_down, shared_gate, shared_up
):
    dps, experts = lax.axis_size("dp"), lax.axis_size("expert")
    groups = pool_pick.shape[0]
    width = tokens.shape[1]
    home_shape, pool_shape = home_pick.shape[:2] + (width,), pool_pick.shape[:2] + (width,)
    bf16 = jnp.bfloat16
    vmem = pl.BlockSpec(memory_space=pltpu.VMEM)
    anywhere = pl.BlockSpec(memory_space=pl.ANY)
    dma = pltpu.SemaphoreType.DMA
    return pl.pallas_call(
        functools.partial(moe_kernel, dps, experts, groups),
        out_shape=(
            jax.ShapeDtypeStruct(home_shape, bf16),
            jax.ShapeDtypeStruct(pool_shape, bf16),
            jax.ShapeDtypeStruct((tokens.shape[0], shared_gate.shape[0]), bf16),
            jax.ShapeDtypeStruct(need.shape, need.dtype),
        ),
        in_specs=[vmem] * 6 + [anywhere] * 3 + [vmem] * 2,
        out_specs=(vmem,) * 4,
        scratch_shapes=[
            pltpu.VMEM((dps * experts,) + need.shape, need.dtype),
            pltpu.VMEM(tokens.shape, bf16),
            pltpu.VMEM(home_shape, bf16),
            pltpu.VMEM(pool_shape, bf16),
            pltpu.VMEM(home_shape, bf16),
            pltpu.VMEM(home_shape, bf16),
            pltpu.VMEM((2,) + pool_shape, bf16),
            pltpu.VMEM(pool_shape, bf16),
            pltpu.VMEM(pool_shape, bf16),
            pltpu.VMEM(pool_shape, bf16),
            pltpu.VMEM(side_out.shape, jnp.float32),
            pltpu.VMEM(w_gate.shape, bf16),
            pltpu.VMEM(w_up.shape, bf16),
            pltpu.VMEM(w_down.shape, bf16),
            dma((3,)),
            dma((4,)),
        ]
        + [dma((dps * experts,))] * 2
        + [dma((experts,))] * 4
        + [dma((groups,))] * 10,
        compiler_params=pltpu.CompilerParams(
            collective_id=0, has_side_effects=True, vmem_limit_bytes=60 * 1024 * 1024
        ),
        name="moe",
    )(home_pick, pool_pick, side_out, need, scale, tokens, w_gate, w_up, w_down, shared_gate, shared_up)


def split_columns(total, step=128):
    out, at = [], 0
    while at < total:
        out.append((at, min(step, total - at)))
        at += step
    return out


def slab_kernel(
    dps,
    experts,
    groups,
    direct,
    pooled,
    id_ref,
    slot_ref,
    keep_ref,
    logit_ref,
    table_ref,
    tok_ref,
    wg_hbm,
    wu_hbm,
    wd_hbm,
    sg_ref,
    su_ref,
    sd_hbm,
    out_ref,
    need_max,
    need_all,
    back,
    shared_slab,
    home_out,
    pool_out,
    home_in,
    pool_in,
    res,
    ret,
    wg,
    wu,
    slab,
    sel_all,
    h_all,
    spread,
    stage,
    w_sem,
    own_sem,
    ns_sem,
    nr_sem,
    hs_sem,
    hr_sem,
    rs_sem,
    rr_sem,
    zs_sem,
    zr_sem,
    xs_sem,
    xr_sem,
    ls_sem,
    lr_sem,
    gs_sem,
    gr_sem,
    os_sem,
    or_sem,
    vs_sem,
    vr_sem,
    ss_sem,
    sr_sem,
):
    my_dp = lax.axis_index("dp")
    e = lax.axis_index("expert")
    g = e // 2
    p = e - 2 * g
    partner = e + 1 - 2 * p
    total = dps * experts
    me = my_dp * experts + e
    members = 2 * dps
    j = p * dps + my_dp
    half = groups // 2
    mate = flip(g, 1, groups)
    far_mid = jnp.where(g < half, half, half - 1)
    far_end = flip(far_mid, 1, groups)
    is_mid = (g == half) | (g == half - 1)
    mid = is_mid.astype(jnp.int32)
    rows, width = tok_ref.shape
    hid = wg.shape[1]
    mix = sg_ref.shape[0]
    spill = table_ref.shape[1]
    base = (direct + 15) // 16 * 16
    stride = base + pooled
    ncols = slab.shape[3]
    chunks = split_columns(ncols)

    barrier = pltpu.get_barrier_semaphore()

    @pl.loop(1, total)
    def _(k):
        there = lax.rem(me + k, total)
        pl.semaphore_signal(
            barrier,
            inc=1,
            device_id={"dp": there // experts, "expert": lax.rem(there, experts)},
            device_id_type=MESH,
        )

    def columns(member, at=0, count=ncols):
        return pl.ds(pl.multiple_of(member * ncols + at, 128), count)

    weights = [
        pltpu.make_async_copy(a, b, w_sem.at[i])
        for i, (a, b) in enumerate(((wg_hbm, wg), (wu_hbm, wu)))
    ]
    own_slab = pltpu.make_async_copy(wd_hbm.at[:, columns(j)], slab.at[g, p], w_sem.at[2])
    own_mix = pltpu.make_async_copy(
        sd_hbm.at[:, columns(j)], shared_slab.at[pl.ds(0, mix)], own_sem.at[2]
    )
    own = [
        pltpu.make_async_copy(home_out.at[e], home_in.at[e], own_sem.at[0]),
        pltpu.make_async_copy(pool_out.at[g], pool_in.at[g, 0], own_sem.at[1]),
    ]

    def remote(src, dst, send, recv, to):
        return pltpu.make_async_remote_copy(
            src_ref=src,
            dst_ref=dst,
            send_sem=send,
            recv_sem=recv,
            device_id=to,
            device_id_type=MESH,
        )

    def n_copy(k):
        there = lax.rem(me + k, total)
        to = {"dp": there // experts, "expert": lax.rem(there, experts)}
        return remote(need_all.at[me], need_all.at[me], ns_sem.at[k], nr_sem.at[k], to)

    def z_copy(k):
        to = flip(g, k, groups)
        there = {"expert": 2 * to + p}
        return remote(pool_out.at[to], pool_in.at[g, 0], zs_sem.at[k], zr_sem.at[k], there)

    def h_copy(k):
        to = flip(e, k, experts)
        return remote(home_out.at[to], home_in.at[e], hs_sem.at[k], hr_sem.at[k], {"expert": to})

    def x_copy(k):
        origin = flip(g, k, groups)
        return remote(
            pool_in.at[origin, 0],
            pool_in.at[flip(g, k, groups), 1],
            xs_sem.at[k],
            xr_sem.at[k],
            {"expert": partner},
        )

    def r_copy(k):
        origin = flip(e, k, experts)
        return remote(res.at[origin], ret.at[e], rs_sem.at[k], rr_sem.at[k], {"expert": origin})

    def peer(k):
        m = flip(j, k, members)
        return m, {"dp": lax.rem(m, dps), "expert": 2 * g + m // dps}

    def l_copy(k):
        return remote(sel_all.at[j], sel_all.at[j], ls_sem.at[k], lr_sem.at[k], peer(k)[1])

    def g_copy(k):
        block, there = (j, peer(k)[1]) if k == 1 or k % 2 == 0 else (peer(k - 1)[0], peer(1)[1])
        return remote(h_all.at[block], h_all.at[block], gs_sem.at[k], gr_sem.at[k], there)

    def o_copy(k, c):
        at, count = chunks[c]
        m, there = peer(k)
        return remote(
            stage.at[m, :, pl.ds(at, count)],
            out_ref.at[:, columns(j, at, count)],
            os_sem.at[k, c],
            or_sem.at[k, c],
            there,
        )

    def v_copy():
        j_there = (1 - p) * dps + my_dp
        return remote(
            wd_hbm.at[:, columns(j_there)],
            slab.at[g, p],
            vs_sem.at[0],
            vr_sem.at[0],
            {"expert": partner},
        )

    def s_copy(block, c, slot, to):
        at, count = chunks[c]
        part = slab.at[block, :, :, pl.ds(at, count)]
        return remote(part, part, ss_sem.at[slot, c], sr_sem.at[block, c], {"expert": 2 * to + p})

    for copy in weights:
        copy.start()
    own_slab.start()
    own_mix.start()

    bf16 = jnp.bfloat16

    def steps(count):
        return lax.broadcasted_iota(jnp.int32, (count, rows), 0)

    def marks_of(count, label):
        return jnp.where(steps(count) == label, 1.0, 0.0)

    with jax.named_scope("routing"):
        ident, slot = id_ref[...], slot_ref[...]
        kept = keep_ref[...] != 0
        scale = jax.nn.sigmoid(logit_ref[...]) * keep_ref[...].astype(jnp.float32)
        levels = marks_of(spill, jnp.maximum(slot - spill, 0)).astype(bf16)
        table = table_ref[...].astype(jnp.float32).astype(bf16)
        hosts = jnp.dot(table, levels, preferred_element_type=jnp.float32)
        host = jnp.sum(hosts * marks_of(experts, ident), axis=0, keepdims=True)
        served = jnp.where(slot >= spill, host.astype(jnp.int32), ident)
        order = lax.broadcasted_iota(jnp.int32, (rows, rows), 1)
        earlier = jnp.where(steps(rows) < order, 1.0, 0.0).astype(bf16)

        def rank_of(count, label):
            marks = marks_of(count, label)
            counts = jnp.dot(marks.astype(bf16), earlier, preferred_element_type=jnp.float32)
            return jnp.sum(marks * counts, axis=0, keepdims=True).astype(jnp.int32)

        direct_rank = rank_of(experts, jnp.where(kept, served, -1))
        over = kept & (direct_rank >= direct)
        pool_rank = rank_of(groups, jnp.where(over, served // 2, -1))
        left = over & (pool_rank >= pooled)
        home_cell = jnp.where(kept & (direct_rank < direct), served * direct + direct_rank, -1)
        pool_cell = jnp.where(
            over & (pool_rank < pooled), (served // 2) * pooled + pool_rank, -1
        )
        placed = kept & ((direct_rank < direct) | (pool_rank < pooled))

    def rows_of(cell, first, count):
        pick = marks_of(count, cell - first)
        factor = jnp.sum(pick * scale, axis=1, keepdims=True)
        chosen = jnp.dot(pick.astype(bf16), tok_ref[...], preferred_element_type=jnp.float32)
        return (chosen * factor).astype(bf16)

    @pl.loop(0, groups)
    def _(to):
        with jax.named_scope("pack_pool"):
            pool_out[to] = rows_of(pool_cell, to * pooled, pooled)

    with jax.named_scope("barrier"):
        pl.semaphore_wait(barrier, total - 1)

    for k in (3 - mid, 2 + mid, 1):
        z_copy(k).start()

    v_copy().start()

    @pl.loop(0, experts)
    def _(i):
        to = flip(e, experts - 1 - i, experts)
        with jax.named_scope("pack_home"):
            home_out[to] = rows_of(home_cell, to * direct, direct)

    with jax.named_scope("shared"):
        tok = tok_ref[...]
        last = (((1,), (1,)), ((), ()))
        shared_gate = lax.dot_general(tok, sg_ref[...], last, preferred_element_type=jnp.float32)
        shared_up = lax.dot_general(tok, su_ref[...], last, preferred_element_type=jnp.float32)
        lanes = sel_all.shape[2]
        marks = jnp.transpose(marks_of(lanes, jnp.where(placed, served + mix, -1)))
        sel_all[j] = marks.astype(bf16)
        sel_all[j, :, :mix] = (jax.nn.silu(shared_gate) * shared_up).astype(bf16)

    with jax.named_scope("tables"):
        res[...] = jnp.zeros_like(res)
        shared_slab[mix:, :] = jnp.zeros((lanes - mix, ncols), bf16)
        spot = jnp.where(direct_rank < direct, direct_rank, base + pool_rank)
        cell = jnp.where(placed, served * stride + spot, -1)
        back[...] = jnp.transpose(marks_of(experts * stride, cell)).astype(bf16)
        missed = jnp.max(jnp.where(left, 1.0, 0.0), axis=1, keepdims=True)
        need_all[me] = jnp.broadcast_to(missed, need_all.shape[1:])

    for copy in own[1:]:
        copy.start()
    own[1].wait()
    x_copy(0).start()

    def pool_relay(k):
        with jax.named_scope("z_wait"):
            z_copy(k).wait_recv()
        x_copy(k).start()

    pool_relay(3 - mid)

    @pl.loop(1, experts)
    def _(i):
        h_copy(experts - i).start()

    own[0].start()
    pool_relay(1)

    @pl.loop(1, total)
    def _(k):
        n_copy(k).start()

    @pl.loop(1, members)
    def _(k):
        l_copy(k).start()

    with jax.named_scope("own_wait"):
        own[0].wait()
        own_mix.wait()

    with jax.named_scope("slab_wait"):
        own_slab.wait()
        v_copy().wait_recv()
    for c in range(len(chunks)):
        s_copy(g, c, 0, mate).start()

    with jax.named_scope("w_wait"):
        for copy in weights:
            copy.wait()

    def hidden_of(x):
        gate_out = jnp.dot(x, wg[...], preferred_element_type=jnp.float32)
        up_out = jnp.dot(x, wu[...], preferred_element_type=jnp.float32)
        return (jax.nn.silu(gate_out) * up_out).astype(jnp.bfloat16)

    with jax.named_scope("ffn_own"):
        res[e, :direct, :] = hidden_of(home_in[e])

    pool_relay(2 + mid)

    @pl.loop(0, groups)
    def _(i):
        k = jnp.where(i == 0, 0, jnp.where(i == 1, 3 - mid, jnp.where(i == 2, 1, 2 + mid)))
        origin = flip(g, k, groups)
        with jax.named_scope("x_wait"):
            x_copy(k).wait_recv()
        with jax.named_scope("ffn_pool"):
            both = hidden_of(pool_in[origin].reshape(2 * pooled, width))
            res[2 * origin + p, base : base + pooled, :] = both[:pooled]
            res[2 * origin + 1 - p, base : base + pooled, :] = both[pooled:]

    own_ret = pltpu.make_async_copy(res.at[e], ret.at[e], own_sem.at[0])
    own_ret.start()

    def home_block(k):
        origin = flip(e, k, experts)
        with jax.named_scope("h_wait"):
            h_copy(k).wait_recv()
        with jax.named_scope("ffn_home"):
            res[origin, :direct, :] = hidden_of(home_in[origin])
        r_copy(k).start()

    @pl.loop(1, experts)
    def _(i):
        home_block(jnp.where(i < experts // 2, experts // 2 - i, experts + experts // 2 - 1 - i))

    def far_start(*which):
        for c in which:
            s_copy(g, c, 1, far_mid).start()

    far_start(*range(min(2, len(chunks))))

    def slab_step(*which):
        @pl.when(is_mid)
        def _():
            for c in which:
                with jax.named_scope("slab_relay"):
                    for slot, block in ((2, far_mid), (3, far_end)):
                        copy = s_copy(block, c, slot, mate)
                        copy.wait_recv()
                        copy.start()

    own_ret.wait()

    with jax.named_scope("ret_wait"):

        @pl.loop(1, experts)
        def _(i):
            r_copy(experts - i).wait_recv()

    with jax.named_scope("find"):
        found = jnp.dot(
            back[...], ret[...].reshape(-1, hid), preferred_element_type=jnp.float32
        )
        h_all[j] = found.astype(jnp.bfloat16)

    for k in [*range(members - 2, 0, -2), 1]:
        g_copy(k).start()

    def expand(m):
        values = h_all[m]
        marks = sel_all[m].astype(jnp.float32)
        for x in range(experts):
            mark = marks[:, mix + x : mix + x + 1] > 0.5
            spread[m, :, x * hid : (x + 1) * hid] = jnp.where(mark, values, jnp.zeros_like(values))

    def slab_arrive(c):
        s_copy(mate, c, 0, mate).wait_recv()

        @pl.when(jnp.logical_not(is_mid))
        def _():
            for block in (far_mid, far_end):
                s_copy(block, c, 2, mate).wait_recv()

    def project(m, c):
        at, count = chunks[c]
        w = slab[:, :, :, at : at + count].reshape(experts * hid, count)
        y = jnp.dot(spread[m], w, preferred_element_type=jnp.float32)
        y += jnp.dot(
            sel_all[m], shared_slab[:, at : at + count], preferred_element_type=jnp.float32
        )
        stage[m, :, at : at + count] = y.astype(jnp.bfloat16)

    with jax.named_scope("expand"):
        expand(j)

    def hidden_arrive(k):
        with jax.named_scope("g_wait"):
            l_copy(k).wait_recv()
            g_copy(k).wait_recv()
        if k % 2 == 0:
            g_copy(k + 1).start()
        with jax.named_scope("expand"):
            expand(peer(k)[0])

    far_start(*range(2, min(3, len(chunks))))
    for k in [1, *range(2, members, 2)]:
        hidden_arrive(k)
        if k == 2:
            far_start(*range(3, min(4, len(chunks))))
            slab_step(0)
    far_start(*range(4, len(chunks)))
    for k in range(3, members, 2):
        hidden_arrive(k)

    def own_out(c):
        at, count = chunks[c]
        return pltpu.make_async_copy(
            stage.at[j, :, pl.ds(at, count)],
            out_ref.at[:, columns(j, at, count)],
            os_sem.at[0, c],
        )

    for c in range(len(chunks)):
        with jax.named_scope("slab_arrive"):
            slab_arrive(c)

        @pl.loop(1, members)
        def _(i):
            k = members - i
            with jax.named_scope("project"):
                project(peer(k)[0], c)
            o_copy(k, c).start()

        project(j, c)
        own_out(c).start()
        if c + 1 < len(chunks):
            slab_step(c + 1)

    for c in range(len(chunks)):

        @pl.loop(1, members)
        def _(k):
            with jax.named_scope("out_wait"):
                o_copy(k, c).wait()

        own_out(c).wait()
        s_copy(g, c, 1, far_mid).wait_send()
        s_copy(g, c, 0, mate).wait_send()

        @pl.when(is_mid)
        def _():
            for slot, block in ((2, far_mid), (3, far_end)):
                s_copy(block, c, slot, mate).wait_send()

    with jax.named_scope("v_wait"):
        v_copy().wait_send()

    @pl.loop(0, groups)
    def _(k):
        x_copy(k).wait_send()

    @pl.loop(1, groups)
    def _(k):
        z_copy(k).wait_send()

    @pl.loop(1, total)
    def _(k):
        n_copy(k).wait()

    @pl.loop(1, members)
    def _(k):
        l_copy(k).wait_send()

    for k in range(1, members):
        g_copy(k).wait_send()

    @pl.loop(1, experts)
    def _(k):
        h_copy(k).wait_send()
        r_copy(k).wait_send()

    need_max[0, 0] = jnp.max(need_all[...])


def slab_exchange(
    direct, pooled, expert_id, token_slot, keep, router_logit, table, tokens, weights, shared
):
    dps, experts = lax.axis_size("dp"), lax.axis_size("expert")
    groups = experts // 2
    rows, width = tokens.shape
    hid = weights[0].shape[1]
    members = 2 * dps
    ncols = width // members
    parts = len(split_columns(ncols))
    cell = (direct + 15) // 16 * 16 + pooled
    bf16 = jnp.bfloat16
    vmem = pl.BlockSpec(memory_space=pltpu.VMEM)
    anywhere = pl.BlockSpec(memory_space=pl.ANY)
    dma = pltpu.SemaphoreType.DMA
    return pl.pallas_call(
        functools.partial(slab_kernel, dps, experts, groups, direct, pooled),
        out_shape=(
            jax.ShapeDtypeStruct((rows, width), bf16),
            jax.ShapeDtypeStruct((1, 1), jnp.float32),
        ),
        in_specs=[vmem] * 6 + [anywhere] * 3 + [vmem] * 2 + [anywhere],
        out_specs=(vmem, pl.BlockSpec(memory_space=pltpu.SMEM)),
        scratch_shapes=[
            pltpu.VMEM((dps * experts, 8, 128), jnp.float32),
            pltpu.VMEM((rows, experts * cell), bf16),
            pltpu.VMEM((128, ncols), bf16),
            pltpu.VMEM((experts, direct, width), bf16),
            pltpu.VMEM((groups, pooled, width), bf16),
            pltpu.VMEM((experts, direct, width), bf16),
            pltpu.VMEM((groups, 2, pooled, width), bf16),
            pltpu.VMEM((experts, cell, hid), bf16),
            pltpu.VMEM((experts, cell, hid), bf16),
            pltpu.VMEM((width, hid), bf16),
            pltpu.VMEM((width, hid), bf16),
            pltpu.VMEM((groups, 2, hid, ncols), bf16),
            pltpu.VMEM((members, rows, 128), bf16),
            pltpu.VMEM((members, rows, hid), bf16),
            pltpu.VMEM((members, rows, experts * hid), bf16),
            pltpu.VMEM((members, rows, ncols), bf16),
            dma((3,)),
            dma((3,)),
        ]
        + [dma((dps * experts,))] * 2
        + [dma((experts,))] * 4
        + [dma((groups,))] * 4
        + [dma((members,))] * 4
        + [dma((members, parts))] * 2
        + [dma((1,))] * 2
        + [dma((4, parts)), dma((groups, parts))],
        compiler_params=pltpu.CompilerParams(
            collective_id=1, has_side_effects=True, vmem_limit_bytes=60 * 1024 * 1024
        ),
        name="slab_moe",
    )(
        *(v.reshape(1, rows) for v in (expert_id, token_slot, keep, router_logit)),
        table,
        tokens,
        *weights,
        shared[0].T,
        shared[1].T,
        shared[2],
    )


def slab_body(direct, pooled, args):
    tokens, router_logit, expert_id, token_slot, keep, table = args[:6]
    weights = tuple(w[0] for w in args[6:9])
    shared_gate, shared_up, shared_down = args[9:]
    out, need = slab_exchange(
        direct,
        pooled,
        expert_id,
        token_slot,
        keep,
        router_logit,
        table,
        tokens,
        weights,
        args[9:],
    )

    def some_left():
        experts = lax.axis_size("expert")
        count, width = tokens.shape
        spill = table.shape[1]
        scale = jax.nn.sigmoid(router_logit) * keep.astype(jnp.float32)
        positions = jnp.arange(count, dtype=jnp.int32)
        is_spill = token_slot >= spill
        level = jnp.maximum(token_slot - spill, 0)
        host = table[expert_id, level]
        served = jnp.where(is_spill, host, expert_id)
        kept = keep != 0
        before = positions[None, :] < positions[:, None]

        def rank_of(member, label):
            same = (label[:, None] == label[None, :]) & member[None, :] & before
            return jnp.sum(same.astype(jnp.int32), axis=1)

        over = kept & (rank_of(kept, served) >= direct)
        left = over & (rank_of(over, served // 2) >= pooled)
        rows = (tokens.astype(jnp.float32) * scale[:, None]).astype(jnp.bfloat16)
        lanes = 3 * spill
        to_right = host == (expert_id + 1) % experts
        lane_index = jnp.where(
            is_spill, spill + level + jnp.where(to_right, 0, spill), token_slot
        )
        cell_index = served * lanes + lane_index
        source_row = jnp.zeros((experts * lanes,), jnp.int32).at[cell_index].set(positions)
        outgoing = rows[source_row].reshape(experts, lanes, width)
        incoming = lax.all_to_all(outgoing, "expert", split_axis=0, concat_axis=0, tiled=True)
        answers = lax.all_to_all(
            expert_ffn(incoming, *weights), "expert", split_axis=0, concat_axis=0, tiled=True
        )
        rest = answers.reshape(-1, width)[cell_index].astype(jnp.float32)
        gate = jnp.dot(tokens, shared_gate, preferred_element_type=jnp.float32)
        up = jnp.dot(tokens, shared_up, preferred_element_type=jnp.float32)
        hidden = (jax.nn.silu(gate) * up).astype(jnp.bfloat16)
        common = jnp.dot(hidden, shared_down, preferred_element_type=jnp.float32)
        return jnp.where(left[:, None], (common + rest).astype(jnp.bfloat16), out)

    return lax.cond(need[0, 0] > 0, some_left, lambda: out)


def body(
    tokens,
    router_logit,
    expert_id,
    token_slot,
    keep,
    overflow_host,
    expert_gate,
    expert_up,
    expert_down,
    shared_gate,
    shared_up,
    shared_down,
):
    experts = lax.axis_size("expert")
    dps = lax.axis_size("dp")
    groups = experts // 2
    tok_count, model_width = tokens.shape
    slot_count = 2 * tok_count // experts
    home_count = slot_count // 2
    spill_count = slot_count - home_count
    direct = max(1, 3 * home_count // 4)
    pooled = home_count
    narrow = shared_gate.shape[1] + experts <= 128 and spill_count == home_count
    even = dps in (2, 4, 8) and model_width % (2 * dps * 128) == 0
    if groups == 4 and even and narrow:
        args = (tokens, router_logit, expert_id, token_slot, keep, overflow_host)
        args += (expert_gate, expert_up, expert_down, shared_gate, shared_up, shared_down)
        return slab_body(direct, pooled, args)
    w_gate, w_up, w_down = expert_gate[0], expert_up[0], expert_down[0]
    token_scale = jax.nn.sigmoid(router_logit) * keep.astype(jnp.float32)
    positions = jnp.arange(tok_count, dtype=jnp.int32)
    is_spill = token_slot >= home_count
    spill_level = jnp.maximum(token_slot - home_count, 0)
    table_index = expert_id * spill_count + spill_level
    table_ids = jnp.arange(experts * spill_count, dtype=jnp.int32)
    host_expert = jnp.sum(
        jnp.where(table_index[:, None] == table_ids[None, :], overflow_host.reshape(1, -1), 0),
        axis=1,
    )
    served = jnp.where(is_spill, host_expert, expert_id)
    kept = keep != 0
    before = positions[None, :] < positions[:, None]

    def rank_of(member, label):
        same = (label[:, None] == label[None, :]) & member[None, :] & before
        return jnp.sum(same.astype(jnp.int32), axis=1)

    direct_rank = rank_of(kept, served)
    over = kept & (direct_rank >= direct)
    pool_rank = rank_of(over, served // 2)
    left = over & (pool_rank >= pooled)
    home_cell = jnp.where(kept & ~over, served * direct + direct_rank, -1)
    pool_cell = jnp.where(over & ~left, (served // 2) * pooled + pool_rank, -1)
    home_ids = jnp.arange(experts * direct, dtype=jnp.int32)
    pool_ids = jnp.arange(groups * pooled, dtype=jnp.int32)
    home_pick = (home_ids[:, None] == home_cell[None, :]).astype(jnp.bfloat16)
    pool_pick = (pool_ids[:, None] == pool_cell[None, :]).astype(jnp.bfloat16)
    unserved = jnp.broadcast_to(jnp.max(left.astype(jnp.int32)), (8, 128))
    side = jnp.sum(
        jnp.where(pool_ids[:, None] == pool_cell[None, :], (served % 2)[None, :], 0), axis=1
    )
    side_out = jnp.broadcast_to(side.astype(jnp.float32)[:, None], (groups * pooled, 128))
    home_ret, pool_ret, shared_hidden, unserved_all = routed_exchange(
        home_pick.reshape(experts, direct, tok_count),
        pool_pick.reshape(groups, pooled, tok_count),
        side_out.reshape(groups, pooled, 128),
        unserved,
        token_scale[:, None],
        tokens,
        w_gate,
        w_up,
        w_down,
        shared_gate.T,
        shared_up.T,
    )

    def combined():
        home_back = (home_cell[:, None] == home_ids[None, :]).astype(jnp.bfloat16)
        pool_back = (pool_cell[:, None] == pool_ids[None, :]).astype(jnp.bfloat16)
        pick = jnp.concatenate([home_back, pool_back, shared_hidden], axis=1)
        source = jnp.concatenate(
            [home_ret.reshape(-1, model_width), pool_ret.reshape(-1, model_width), shared_down],
            axis=0,
        )
        return jnp.dot(pick, source, preferred_element_type=jnp.float32)

    def all_served():
        return combined().astype(jnp.bfloat16)

    def some_left():
        rows = (tokens.astype(jnp.float32) * token_scale[:, None]).astype(jnp.bfloat16)
        lanes = home_count + 2 * spill_count
        to_right = host_expert == (expert_id + 1) % experts
        lane_index = jnp.where(
            is_spill,
            home_count + spill_level + jnp.where(to_right, 0, spill_count),
            token_slot,
        )
        cell_index = served * lanes + lane_index
        source_row = jnp.zeros((experts * lanes,), jnp.int32).at[cell_index].set(positions)
        outgoing = rows[source_row].reshape(experts, lanes, model_width)
        incoming = lax.all_to_all(outgoing, "expert", split_axis=0, concat_axis=0, tiled=True)
        answers = lax.all_to_all(
            expert_ffn(incoming, w_gate, w_up, w_down),
            "expert",
            split_axis=0,
            concat_axis=0,
            tiled=True,
        )
        rest = answers.reshape(-1, model_width)[cell_index].astype(jnp.float32)
        return (combined() + jnp.where(left[:, None], rest, 0.0)).astype(jnp.bfloat16)

    return lax.cond(unserved_all[0, 0] > 0, some_left, all_served)


def solution(mesh):
    return jax.shard_map(
        body,
        mesh=mesh,
        in_specs=(
            P(("dp", "expert"), None),
            P(("dp", "expert")),
            P(("dp", "expert")),
            P(("dp", "expert")),
            P(("dp", "expert")),
            P(),
            P("expert", None, None),
            P("expert", None, None),
            P("expert", None, None),
            P(),
            P(),
            P(),
        ),
        out_specs=P(("dp", "expert"), None),
        check_vma=False,
    )
```

```python
import functools

import jax
import jax.numpy as jnp
from jax import lax
from jax.experimental import pallas as pl
from jax.experimental.pallas import tpu as pltpu
from jax.sharding import PartitionSpec as P

MESH = pl.DeviceIdType.MESH


def expert_ffn(inputs, w_gate, w_up, w_down):
    flat_rows = inputs.reshape(-1, inputs.shape[-1])
    gate_out = jnp.dot(flat_rows, w_gate, preferred_element_type=jnp.float32)
    up_out = jnp.dot(flat_rows, w_up, preferred_element_type=jnp.float32)
    hidden = (jax.nn.silu(gate_out) * up_out).astype(jnp.bfloat16)
    result = jnp.dot(hidden, w_down, preferred_element_type=jnp.float32).astype(jnp.bfloat16)
    return result.reshape(inputs.shape)


def flip(index, step, count):
    out, bit = 0, 1
    while bit < count:
        out = out + bit * lax.rem(index // bit + step // bit, 2)
        bit *= 2
    return out


def moe_kernel(
    dps,
    experts,
    groups,
    home_pick,
    pool_pick,
    side_out,
    need_ref,
    scale_ref,
    tok_ref,
    wg_hbm,
    wu_hbm,
    wd_hbm,
    sg_ref,
    su_ref,
    home_ret,
    pool_ret,
    shared_ref,
    need_max,
    need_all,
    routed_in,
    home_out,
    pool_out,
    home_in,
    home_res,
    pool_in,
    pool_res,
    pool_part,
    pool_comb,
    side_in,
    wg,
    wu,
    wd,
    w_sem,
    own_sem,
    ns_sem,
    nr_sem,
    hs_sem,
    hr_sem,
    rs_sem,
    rr_sem,
    zs_sem,
    zr_sem,
    ms_sem,
    mr_sem,
    xs_sem,
    xr_sem,
    ps_sem,
    pr_sem,
    cs_sem,
    cr_sem,
):
    my_dp = lax.axis_index("dp")
    e = lax.axis_index("expert")
    g = e // 2
    p = e - 2 * g
    partner = e + 1 - 2 * p
    total = dps * experts
    me = my_dp * experts + e

    barrier = pltpu.get_barrier_semaphore()

    @pl.loop(1, total)
    def _(k):
        there = lax.rem(me + k, total)
        pl.semaphore_signal(
            barrier,
            inc=1,
            device_id={"dp": there // experts, "expert": lax.rem(there, experts)},
            device_id_type=MESH,
        )

    weights = [
        pltpu.make_async_copy(a, b, w_sem.at[i])
        for i, (a, b) in enumerate(((wg_hbm, wg), (wu_hbm, wu), (wd_hbm, wd)))
    ]
    own = [
        pltpu.make_async_copy(home_out.at[e], home_in.at[e], own_sem.at[0]),
        pltpu.make_async_copy(pool_out.at[g], pool_in.at[0, g], own_sem.at[1]),
        pltpu.make_async_copy(side_out.at[g], side_in.at[g], own_sem.at[2]),
        pltpu.make_async_copy(need_ref, need_all.at[me], own_sem.at[3]),
    ]

    def remote(src, dst, send, recv, to):
        return pltpu.make_async_remote_copy(
            src_ref=src,
            dst_ref=dst,
            send_sem=send,
            recv_sem=recv,
            device_id={"expert": to},
            device_id_type=MESH,
        )

    def n_copy(k):
        there = lax.rem(me + k, total)
        return pltpu.make_async_remote_copy(
            src_ref=need_ref,
            dst_ref=need_all.at[me],
            send_sem=ns_sem.at[k],
            recv_sem=nr_sem.at[k],
            device_id={"dp": there // experts, "expert": lax.rem(there, experts)},
            device_id_type=MESH,
        )

    def z_copy(k):
        to = flip(g, k, groups)
        return remote(pool_out.at[to], pool_in.at[0, g], zs_sem.at[k], zr_sem.at[k], 2 * to + p)

    def m_copy(k):
        to = flip(g, k, groups)
        return remote(side_out.at[to], side_in.at[g], ms_sem.at[k], mr_sem.at[k], 2 * to + p)

    def h_copy(k):
        to = flip(e, k, experts)
        return remote(home_out.at[to], home_in.at[e], hs_sem.at[k], hr_sem.at[k], to)

    def x_copy(k):
        origin = flip(g, k, groups)
        return remote(
            pool_in.at[0, origin],
            pool_in.at[1, flip(g, k, groups)],
            xs_sem.at[k],
            xr_sem.at[k],
            partner,
        )

    def p_copy(k):
        origin = flip(g, k, groups)
        return remote(
            pool_res.at[origin], pool_part.at[origin], ps_sem.at[k], pr_sem.at[k], partner
        )

    def c_copy(k):
        origin = flip(g, k, groups)
        return remote(
            pool_comb.at[origin], pool_ret.at[g], cs_sem.at[k], cr_sem.at[k], 2 * origin + p
        )

    def r_copy(k):
        origin = flip(e, k, experts)
        return remote(home_res.at[origin], home_ret.at[e], rs_sem.at[k], rr_sem.at[k], origin)

    def rows_of(pick):
        return jnp.dot(pick, routed_in[...], preferred_element_type=jnp.float32).astype(jnp.bfloat16)

    routed_in[...] = (tok_ref[...].astype(jnp.float32) * scale_ref[...]).astype(jnp.bfloat16)

    pl.semaphore_wait(barrier, total - 1)

    @pl.loop(1, groups + 1)
    def _(i):
        k = groups - i
        to = flip(g, k, groups)
        pool_out[to] = rows_of(pool_pick[to])

        @pl.when(i > 1)
        def _():
            z_copy(k + 1).start()
            m_copy(k + 1).start()

    @pl.loop(1, experts + 1)
    def _(i):
        k = experts - i
        to = flip(e, k, experts)
        home_out[to] = rows_of(home_pick[to])

        @pl.when(i > 1)
        def _():
            h_copy(k + 1).start()

    for copy in own:
        copy.start()
    for copy in weights:
        copy.start()

    @pl.loop(1, total)
    def _(k):
        n_copy(k).start()

    for copy in own:
        copy.wait()
    x_copy(0).start()

    tok = tok_ref[...]
    last = (((1,), (1,)), ((), ()))
    shared_gate = lax.dot_general(tok, sg_ref[...], last, preferred_element_type=jnp.float32)
    shared_up = lax.dot_general(tok, su_ref[...], last, preferred_element_type=jnp.float32)
    shared_ref[...] = (jax.nn.silu(shared_gate) * shared_up).astype(jnp.bfloat16)

    for copy in weights:
        copy.wait()

    def ffn(x):
        gate_out = jnp.dot(x, wg[...], preferred_element_type=jnp.float32)
        up_out = jnp.dot(x, wu[...], preferred_element_type=jnp.float32)
        hidden = (jax.nn.silu(gate_out) * up_out).astype(jnp.bfloat16)
        return jnp.dot(hidden, wd[...], preferred_element_type=jnp.float32).astype(jnp.bfloat16)

    home_res[e] = ffn(home_in[e])
    own_ret = pltpu.make_async_copy(home_res.at[e], home_ret.at[e], own_sem.at[0])
    own_ret.start()

    @pl.loop(1, groups)
    def _(i):
        k = groups - i
        z_copy(k).wait_recv()
        x_copy(k).start()

    def home_block(i):
        k = experts - i
        origin = flip(e, k, experts)
        h_copy(k).wait_recv()
        home_res[origin] = ffn(home_in[origin])
        r_copy(k).start()

    @pl.loop(1, groups + 1)
    def _(i):
        k = groups - i
        origin = flip(g, k, groups)
        x_copy(k).wait_recv()
        pool_res[origin] = ffn(pool_in[1, origin])
        p_copy(k).start()

    @pl.loop(1, groups + 1)
    def _(i):
        k = groups - i
        origin = flip(g, k, groups)
        mine = ffn(pool_in[0, origin])
        p_copy(k).wait_recv()

        @pl.when(k > 0)
        def _():
            m_copy(k).wait_recv()

        here = jnp.abs(side_in[origin][:, :1] - p.astype(jnp.float32)) < 0.5
        pool_comb[origin] = jnp.where(here, mine, pool_part[origin])

        @pl.when(k > 0)
        def _():
            c_copy(k).start()

    own_back = pltpu.make_async_copy(pool_comb.at[g], pool_ret.at[g], own_sem.at[1])
    own_back.start()

    pl.loop(1, experts)(home_block)

    @pl.loop(0, groups)
    def _(k):
        x_copy(k).wait_send()
        p_copy(k).wait_send()

    @pl.loop(1, groups)
    def _(k):
        z_copy(k).wait_send()
        m_copy(k).wait_send()
        c_copy(k).wait()

    @pl.loop(1, total)
    def _(k):
        n_copy(k).wait()

    @pl.loop(1, experts)
    def _(k):
        h_copy(k).wait_send()
        r_copy(k).wait()

    own_ret.wait()
    own_back.wait()
    need_max[...] = jnp.max(need_all[...], axis=0)


def routed_exchange(
    home_pick, pool_pick, side_out, need, scale, tokens, w_gate, w_up, w_down, shared_gate, shared_up
):
    dps, experts = lax.axis_size("dp"), lax.axis_size("expert")
    groups = pool_pick.shape[0]
    width = tokens.shape[1]
    home_shape, pool_shape = home_pick.shape[:2] + (width,), pool_pick.shape[:2] + (width,)
    bf16 = jnp.bfloat16
    vmem = pl.BlockSpec(memory_space=pltpu.VMEM)
    anywhere = pl.BlockSpec(memory_space=pl.ANY)
    dma = pltpu.SemaphoreType.DMA
    return pl.pallas_call(
        functools.partial(moe_kernel, dps, experts, groups),
        out_shape=(
            jax.ShapeDtypeStruct(home_shape, bf16),
            jax.ShapeDtypeStruct(pool_shape, bf16),
            jax.ShapeDtypeStruct((tokens.shape[0], shared_gate.shape[0]), bf16),
            jax.ShapeDtypeStruct(need.shape, need.dtype),
        ),
        in_specs=[vmem] * 6 + [anywhere] * 3 + [vmem] * 2,
        out_specs=(vmem,) * 4,
        scratch_shapes=[
            pltpu.VMEM((dps * experts,) + need.shape, need.dtype),
            pltpu.VMEM(tokens.shape, bf16),
            pltpu.VMEM(home_shape, bf16),
            pltpu.VMEM(pool_shape, bf16),
            pltpu.VMEM(home_shape, bf16),
            pltpu.VMEM(home_shape, bf16),
            pltpu.VMEM((2,) + pool_shape, bf16),
            pltpu.VMEM(pool_shape, bf16),
            pltpu.VMEM(pool_shape, bf16),
            pltpu.VMEM(pool_shape, bf16),
            pltpu.VMEM(side_out.shape, jnp.float32),
            pltpu.VMEM(w_gate.shape, bf16),
            pltpu.VMEM(w_up.shape, bf16),
            pltpu.VMEM(w_down.shape, bf16),
            dma((3,)),
            dma((4,)),
        ]
        + [dma((dps * experts,))] * 2
        + [dma((experts,))] * 4
        + [dma((groups,))] * 10,
        compiler_params=pltpu.CompilerParams(
            collective_id=0, has_side_effects=True, vmem_limit_bytes=60 * 1024 * 1024
        ),
        name="moe",
    )(home_pick, pool_pick, side_out, need, scale, tokens, w_gate, w_up, w_down, shared_gate, shared_up)


def split_columns(total, step=128):
    out, at = [], 0
    while at < total:
        out.append((at, min(step, total - at)))
        at += step
    return out


def slab_kernel(
    dps,
    experts,
    groups,
    direct,
    pooled,
    id_ref,
    slot_ref,
    keep_ref,
    logit_ref,
    table_ref,
    tok_ref,
    wg_hbm,
    wu_hbm,
    wd_hbm,
    sg_ref,
    su_ref,
    sd_hbm,
    out_ref,
    need_max,
    need_part,
    need_all,
    back,
    shared_slab,
    home_out,
    pool_out,
    home_in,
    pool_in,
    res,
    ret,
    wg,
    wu,
    slab,
    sel_all,
    h_all,
    spread,
    stage,
    w_sem,
    own_sem,
    ns_sem,
    nr_sem,
    ds_sem,
    dr_sem,
    hs_sem,
    hr_sem,
    rs_sem,
    rr_sem,
    zs_sem,
    zr_sem,
    xs_sem,
    xr_sem,
    ls_sem,
    lr_sem,
    gs_sem,
    gr_sem,
    os_sem,
    or_sem,
    vs_sem,
    vr_sem,
    ss_sem,
    sr_sem,
):
    my_dp = lax.axis_index("dp")
    e = lax.axis_index("expert")
    g = e // 2
    p = e - 2 * g
    partner = e + 1 - 2 * p
    members = 2 * dps
    j = p * dps + my_dp
    half = groups // 2
    mate = flip(g, 1, groups)
    far_mid = jnp.where(g < half, half, half - 1)
    far_end = flip(far_mid, 1, groups)
    is_mid = (g == half) | (g == half - 1)
    mid = is_mid.astype(jnp.int32)
    rows, width = tok_ref.shape
    hid = wg.shape[1]
    mix = sg_ref.shape[0]
    spill = table_ref.shape[1]
    base = (direct + 15) // 16 * 16
    stride = base + pooled
    ncols = slab.shape[3]
    chunks = split_columns(ncols)

    barrier = pltpu.get_barrier_semaphore()

    @pl.loop(1, experts)
    def _(k):
        there = {"expert": flip(e, k, experts)}
        pl.semaphore_signal(barrier, inc=1, device_id=there, device_id_type=MESH)

    def peer(k):
        m = flip(j, k, members)
        return m, {"dp": lax.rem(m, dps), "expert": 2 * g + m // dps}

    strangers = [k for k in range(1, members) if k != dps]
    for k in strangers:
        pl.semaphore_signal(barrier, inc=1, device_id=peer(k)[1], device_id_type=MESH)

    def columns(member, at=0, count=ncols):
        return pl.ds(pl.multiple_of(member * ncols + at, 128), count)

    weights = [
        pltpu.make_async_copy(a, b, w_sem.at[i])
        for i, (a, b) in enumerate(((wg_hbm, wg), (wu_hbm, wu)))
    ]
    own_slab = pltpu.make_async_copy(wd_hbm.at[:, columns(j)], slab.at[g, p], w_sem.at[2])
    own_mix = pltpu.make_async_copy(
        sd_hbm.at[:, columns(j)], shared_slab.at[pl.ds(0, mix)], own_sem.at[2]
    )
    own = [
        pltpu.make_async_copy(home_out.at[e], home_in.at[e], own_sem.at[0]),
        pltpu.make_async_copy(pool_out.at[g], pool_in.at[g, 0], own_sem.at[1]),
    ]

    def remote(src, dst, send, recv, to):
        return pltpu.make_async_remote_copy(
            src_ref=src,
            dst_ref=dst,
            send_sem=send,
            recv_sem=recv,
            device_id=to,
            device_id_type=MESH,
        )

    def n_copy(k):
        there = {"expert": flip(e, k, experts)}
        return remote(need_part.at[e], need_part.at[e], ns_sem.at[k], nr_sem.at[k], there)

    def d_copy(k):
        there = {"dp": flip(my_dp, k, dps)}
        part = need_all.at[my_dp]
        return remote(part, part, ds_sem.at[k], dr_sem.at[k], there)

    def z_copy(k):
        to = flip(g, k, groups)
        there = {"expert": 2 * to + p}
        return remote(pool_out.at[to], pool_in.at[g, 0], zs_sem.at[k], zr_sem.at[k], there)

    def h_copy(k):
        to = flip(e, k, experts)
        return remote(home_out.at[to], home_in.at[e], hs_sem.at[k], hr_sem.at[k], {"expert": to})

    def x_copy(k):
        origin = flip(g, k, groups)
        return remote(
            pool_in.at[origin, 0],
            pool_in.at[flip(g, k, groups), 1],
            xs_sem.at[k],
            xr_sem.at[k],
            {"expert": partner},
        )

    def r_copy(k):
        origin = flip(e, k, experts)
        return remote(res.at[origin], ret.at[e], rs_sem.at[k], rr_sem.at[k], {"expert": origin})

    def l_copy(k):
        return remote(sel_all.at[j], sel_all.at[j], ls_sem.at[k], lr_sem.at[k], peer(k)[1])

    def g_copy(k):
        block, there = (j, peer(k)[1]) if k == 1 or k % 2 == 0 else (peer(k - 1)[0], peer(1)[1])
        return remote(h_all.at[block], h_all.at[block], gs_sem.at[k], gr_sem.at[k], there)

    def o_copy(k, c):
        at, count = chunks[c]
        m, there = peer(k)
        return remote(
            stage.at[m, :, pl.ds(at, count)],
            out_ref.at[:, columns(j, at, count)],
            os_sem.at[k, c],
            or_sem.at[k, c],
            there,
        )

    def v_copy():
        j_there = (1 - p) * dps + my_dp
        return remote(
            wd_hbm.at[:, columns(j_there)],
            slab.at[g, p],
            vs_sem.at[0],
            vr_sem.at[0],
            {"expert": partner},
        )

    def s_copy(block, c, slot, to):
        at, count = chunks[c]
        part = slab.at[block, :, :, pl.ds(at, count)]
        return remote(part, part, ss_sem.at[slot, c], sr_sem.at[block, c], {"expert": 2 * to + p})

    for copy in weights:
        copy.start()
    own_slab.start()
    own_mix.start()

    bf16 = jnp.bfloat16

    def steps(count):
        return lax.broadcasted_iota(jnp.int32, (count, rows), 0)

    def marks_of(count, label):
        return jnp.where(steps(count) == label, 1.0, 0.0)

    with jax.named_scope("routing"):
        ident, slot = id_ref[...], slot_ref[...]
        kept = keep_ref[...] != 0
        scale = jax.nn.sigmoid(logit_ref[...]) * keep_ref[...].astype(jnp.float32)
        levels = marks_of(spill, jnp.maximum(slot - spill, 0)).astype(bf16)
        table = table_ref[...].astype(jnp.float32).astype(bf16)
        hosts = jnp.dot(table, levels, preferred_element_type=jnp.float32)
        host = jnp.sum(hosts * marks_of(experts, ident), axis=0, keepdims=True)
        served = jnp.where(slot >= spill, host.astype(jnp.int32), ident)
        order = lax.broadcasted_iota(jnp.int32, (rows, rows), 1)
        earlier = jnp.where(steps(rows) < order, 1.0, 0.0).astype(bf16)

        def rank_of(count, label):
            marks = marks_of(count, label)
            counts = jnp.dot(marks.astype(bf16), earlier, preferred_element_type=jnp.float32)
            return jnp.sum(marks * counts, axis=0, keepdims=True).astype(jnp.int32)

        direct_rank = rank_of(experts, jnp.where(kept, served, -1))
        over = kept & (direct_rank >= direct)
        pool_rank = rank_of(groups, jnp.where(over, served // 2, -1))
        left = over & (pool_rank >= pooled)
        home_cell = jnp.where(kept & (direct_rank < direct), served * direct + direct_rank, -1)
        pool_cell = jnp.where(
            over & (pool_rank < pooled), (served // 2) * pooled + pool_rank, -1
        )
        placed = kept & ((direct_rank < direct) | (pool_rank < pooled))

    def rows_of(cell, first, count):
        pick = marks_of(count, cell - first)
        factor = jnp.sum(pick * scale, axis=1, keepdims=True)
        chosen = jnp.dot(pick.astype(bf16), tok_ref[...], preferred_element_type=jnp.float32)
        return (chosen * factor).astype(bf16)

    @pl.loop(0, groups)
    def _(to):
        with jax.named_scope("pack_pool"):
            pool_out[to] = rows_of(pool_cell, to * pooled, pooled)

    with jax.named_scope("barrier"):
        pl.semaphore_wait(barrier, experts - 1 + len(strangers))

    for k in (3 - mid, 2 + mid, 1):
        z_copy(k).start()

    v_copy().start()

    @pl.loop(0, experts)
    def _(i):
        to = flip(e, experts - 1 - i, experts)
        with jax.named_scope("pack_home"):
            home_out[to] = rows_of(home_cell, to * direct, direct)

    with jax.named_scope("shared"):
        tok = tok_ref[...]
        last = (((1,), (1,)), ((), ()))
        shared_gate = lax.dot_general(tok, sg_ref[...], last, preferred_element_type=jnp.float32)
        shared_up = lax.dot_general(tok, su_ref[...], last, preferred_element_type=jnp.float32)
        lanes = sel_all.shape[2]
        marks = jnp.transpose(marks_of(lanes, jnp.where(placed, served + mix, -1)))
        sel_all[j] = marks.astype(bf16)
        sel_all[j, :, :mix] = (jax.nn.silu(shared_gate) * shared_up).astype(bf16)

    with jax.named_scope("tables"):
        res[...] = jnp.zeros_like(res)
        shared_slab[mix:, :] = jnp.zeros((lanes - mix, ncols), bf16)
        spot = jnp.where(direct_rank < direct, direct_rank, base + pool_rank)
        cell = jnp.where(placed, served * stride + spot, -1)
        back[...] = jnp.transpose(marks_of(experts * stride, cell)).astype(bf16)
        missed = jnp.max(jnp.where(left, 1.0, 0.0), axis=1, keepdims=True)
        need_part[e] = jnp.broadcast_to(missed, need_part.shape[1:])

    for copy in own[1:]:
        copy.start()
    own[1].wait()
    x_copy(0).start()

    def pool_relay(k):
        with jax.named_scope("z_wait"):
            z_copy(k).wait_recv()
        x_copy(k).start()

    pool_relay(3 - mid)

    @pl.loop(1, experts)
    def _(i):
        h_copy(experts - i).start()

    own[0].start()
    pool_relay(1)

    @pl.loop(1, experts)
    def _(k):
        n_copy(k).start()

    @pl.loop(1, members)
    def _(k):
        l_copy(k).start()

    with jax.named_scope("own_wait"):
        own[0].wait()
        own_mix.wait()

    with jax.named_scope("slab_wait"):
        own_slab.wait()
        v_copy().wait_recv()
    for c in range(len(chunks)):
        s_copy(g, c, 0, mate).start()

    with jax.named_scope("w_wait"):
        for copy in weights:
            copy.wait()

    def hidden_of(x):
        gate_out = jnp.dot(x, wg[...], preferred_element_type=jnp.float32)
        up_out = jnp.dot(x, wu[...], preferred_element_type=jnp.float32)
        return (jax.nn.silu(gate_out) * up_out).astype(jnp.bfloat16)

    with jax.named_scope("ffn_own"):
        res[e, :direct, :] = hidden_of(home_in[e])

    pool_relay(2 + mid)

    @pl.loop(0, groups)
    def _(i):
        k = jnp.where(i == 0, 0, jnp.where(i == 1, 3 - mid, jnp.where(i == 2, 1, 2 + mid)))
        origin = flip(g, k, groups)
        with jax.named_scope("x_wait"):
            x_copy(k).wait_recv()
        with jax.named_scope("ffn_pool"):
            both = hidden_of(pool_in[origin].reshape(2 * pooled, width))
            res[2 * origin + p, base : base + pooled, :] = both[:pooled]
            res[2 * origin + 1 - p, base : base + pooled, :] = both[pooled:]

    own_ret = pltpu.make_async_copy(res.at[e], ret.at[e], own_sem.at[0])
    own_ret.start()

    def home_block(k):
        origin = flip(e, k, experts)
        with jax.named_scope("h_wait"):
            h_copy(k).wait_recv()
        with jax.named_scope("ffn_home"):
            res[origin, :direct, :] = hidden_of(home_in[origin])
        r_copy(k).start()

    @pl.loop(1, experts)
    def _(i):
        home_block(jnp.where(i < experts // 2, experts // 2 - i, experts + experts // 2 - 1 - i))

    def far_start(*which):
        for c in which:
            s_copy(g, c, 1, far_mid).start()

    far_start(0)

    def slab_step(*which):
        @pl.when(is_mid)
        def _():
            for c in which:
                with jax.named_scope("slab_relay"):
                    for slot, block in ((2, far_mid), (3, far_end)):
                        copy = s_copy(block, c, slot, mate)
                        copy.wait_recv()
                        copy.start()

    own_ret.wait()

    with jax.named_scope("ret_wait"):

        @pl.loop(1, experts)
        def _(i):
            r_copy(experts - i).wait_recv()

    far_start(*range(1, min(2, len(chunks))))

    with jax.named_scope("find"):
        found = jnp.dot(
            back[...], ret[...].reshape(-1, hid), preferred_element_type=jnp.float32
        )
        h_all[j] = found.astype(jnp.bfloat16)

    for k in [*range(members - 2, 0, -2), 1]:
        g_copy(k).start()

    def expand(m):
        values = h_all[m]
        marks = sel_all[m].astype(jnp.float32)
        for x in range(experts):
            mark = marks[:, mix + x : mix + x + 1] > 0.5
            spread[m, :, x * hid : (x + 1) * hid] = jnp.where(mark, values, jnp.zeros_like(values))

    def slab_arrive(c):
        s_copy(mate, c, 0, mate).wait_recv()

        @pl.when(jnp.logical_not(is_mid))
        def _():
            for block in (far_mid, far_end):
                s_copy(block, c, 2, mate).wait_recv()

    def project(m, c):
        at, count = chunks[c]
        w = slab[:, :, :, at : at + count].reshape(experts * hid, count)
        y = jnp.dot(spread[m], w, preferred_element_type=jnp.float32).astype(bf16)
        common = shared_slab[:, at : at + count]
        common = jnp.dot(sel_all[m], common, preferred_element_type=jnp.float32)
        stage[m, :, at : at + count] = (y.astype(jnp.float32) + common).astype(bf16)

    with jax.named_scope("expand"):
        expand(j)

    def hidden_arrive(k):
        with jax.named_scope("g_wait"):
            l_copy(k).wait_recv()
            g_copy(k).wait_recv()
        if k % 2 == 0:
            g_copy(k + 1).start()
        with jax.named_scope("expand"):
            expand(peer(k)[0])

    hidden_arrive(1)
    hidden_arrive(2)
    for k in range(4, members, 2):
        hidden_arrive(k)
    slab_step(0)
    far_start(*range(2, min(3, len(chunks))))
    for k in range(3, members, 2):
        hidden_arrive(k)
    slab_step(1)

    @pl.loop(1, experts)
    def _(k):
        n_copy(k).wait_recv()

    need_all[my_dp] = jnp.max(need_part[...], axis=0)

    @pl.loop(1, dps)
    def _(k):
        d_copy(k).start()

    def own_out(c):
        at, count = chunks[c]
        return pltpu.make_async_copy(
            stage.at[j, :, pl.ds(at, count)],
            out_ref.at[:, columns(j, at, count)],
            os_sem.at[0, c],
        )

    for c in range(len(chunks)):
        with jax.named_scope("slab_arrive"):
            slab_arrive(c)

        def send_out(i):
            k = members - i
            with jax.named_scope("project"):
                project(peer(k)[0], c)
            o_copy(k, c).start()

        pl.loop(1, members // 2)(send_out)
        if c < 2:
            far_start(*range(3 + c, min(4 + c, len(chunks)) if c == 0 else len(chunks)))
        pl.loop(members // 2, members)(send_out)

        project(j, c)
        own_out(c).start()
        if c + 2 < len(chunks):
            slab_step(c + 2)

    for c in range(len(chunks)):

        @pl.loop(1, members)
        def _(k):
            with jax.named_scope("out_wait"):
                o_copy(k, c).wait()

        own_out(c).wait()
        s_copy(g, c, 1, far_mid).wait_send()
        s_copy(g, c, 0, mate).wait_send()

        @pl.when(is_mid)
        def _():
            for slot, block in ((2, far_mid), (3, far_end)):
                s_copy(block, c, slot, mate).wait_send()

    with jax.named_scope("v_wait"):
        v_copy().wait_send()

    @pl.loop(0, groups)
    def _(k):
        x_copy(k).wait_send()

    @pl.loop(1, groups)
    def _(k):
        z_copy(k).wait_send()

    @pl.loop(1, experts)
    def _(k):
        n_copy(k).wait_send()

    @pl.loop(1, dps)
    def _(k):
        d_copy(k).wait()

    @pl.loop(1, members)
    def _(k):
        l_copy(k).wait_send()

    for k in range(1, members):
        g_copy(k).wait_send()

    @pl.loop(1, experts)
    def _(k):
        h_copy(k).wait_send()
        r_copy(k).wait_send()

    need_max[0, 0] = jnp.max(need_all[...])


def slab_exchange(
    direct, pooled, expert_id, token_slot, keep, router_logit, table, tokens, weights, shared
):
    dps, experts = lax.axis_size("dp"), lax.axis_size("expert")
    groups = experts // 2
    rows, width = tokens.shape
    hid = weights[0].shape[1]
    members = 2 * dps
    ncols = width // members
    parts = len(split_columns(ncols))
    cell = (direct + 15) // 16 * 16 + pooled
    bf16 = jnp.bfloat16
    vmem = pl.BlockSpec(memory_space=pltpu.VMEM)
    anywhere = pl.BlockSpec(memory_space=pl.ANY)
    dma = pltpu.SemaphoreType.DMA
    return pl.pallas_call(
        functools.partial(slab_kernel, dps, experts, groups, direct, pooled),
        out_shape=(
            jax.ShapeDtypeStruct((rows, width), bf16),
            jax.ShapeDtypeStruct((1, 1), jnp.float32),
        ),
        in_specs=[vmem] * 6 + [anywhere] * 3 + [vmem] * 2 + [anywhere],
        out_specs=(vmem, pl.BlockSpec(memory_space=pltpu.SMEM)),
        scratch_shapes=[
            pltpu.VMEM((experts, 8, 128), jnp.float32),
            pltpu.VMEM((dps, 8, 128), jnp.float32),
            pltpu.VMEM((rows, experts * cell), bf16),
            pltpu.VMEM((128, ncols), bf16),
            pltpu.VMEM((experts, direct, width), bf16),
            pltpu.VMEM((groups, pooled, width), bf16),
            pltpu.VMEM((experts, direct, width), bf16),
            pltpu.VMEM((groups, 2, pooled, width), bf16),
            pltpu.VMEM((experts, cell, hid), bf16),
            pltpu.VMEM((experts, cell, hid), bf16),
            pltpu.VMEM((width, hid), bf16),
            pltpu.VMEM((width, hid), bf16),
            pltpu.VMEM((groups, 2, hid, ncols), bf16),
            pltpu.VMEM((members, rows, 128), bf16),
            pltpu.VMEM((members, rows, hid), bf16),
            pltpu.VMEM((members, rows, experts * hid), bf16),
            pltpu.VMEM((members, rows, ncols), bf16),
            dma((3,)),
            dma((3,)),
        ]
        + [dma((experts,))] * 2
        + [dma((dps,))] * 2
        + [dma((experts,))] * 4
        + [dma((groups,))] * 4
        + [dma((members,))] * 4
        + [dma((members, parts))] * 2
        + [dma((1,))] * 2
        + [dma((4, parts)), dma((groups, parts))],
        compiler_params=pltpu.CompilerParams(
            collective_id=1, has_side_effects=True, vmem_limit_bytes=60 * 1024 * 1024
        ),
        name="slab_moe",
    )(
        *(v.reshape(1, rows) for v in (expert_id, token_slot, keep, router_logit)),
        table,
        tokens,
        *weights,
        shared[0].T,
        shared[1].T,
        shared[2],
    )


def hand_over_kernel(parts, src, dst, sem):
    rows = src.shape[0] // parts

    def copy(i):
        here = pl.ds(i * rows, rows)
        return pltpu.make_async_copy(src.at[here], dst.at[here], sem.at[i])

    for i in range(parts):
        copy(i).start()
    for i in range(parts):
        copy(i).wait()


def hand_over(values):
    parts = 4
    return pl.pallas_call(
        functools.partial(hand_over_kernel, parts),
        out_shape=jax.ShapeDtypeStruct(values.shape, values.dtype),
        in_specs=[pl.BlockSpec(memory_space=pltpu.VMEM)],
        out_specs=pl.BlockSpec(memory_space=pl.ANY),
        scratch_shapes=[pltpu.SemaphoreType.DMA((parts,))],
        compiler_params=pltpu.CompilerParams(vmem_limit_bytes=4 * 1024 * 1024),
        name="hand_over",
    )(values)


def slab_body(direct, pooled, args):
    tokens, router_logit, expert_id, token_slot, keep, table = args[:6]
    weights = tuple(w[0] for w in args[6:9])
    shared_gate, shared_up, shared_down = args[9:]
    out, need = slab_exchange(
        direct,
        pooled,
        expert_id,
        token_slot,
        keep,
        router_logit,
        table,
        tokens,
        weights,
        args[9:],
    )

    def some_left():
        experts = lax.axis_size("expert")
        count, width = tokens.shape
        spill = table.shape[1]
        scale = jax.nn.sigmoid(router_logit) * keep.astype(jnp.float32)
        positions = jnp.arange(count, dtype=jnp.int32)
        is_spill = token_slot >= spill
        level = jnp.maximum(token_slot - spill, 0)
        host = table[expert_id, level]
        served = jnp.where(is_spill, host, expert_id)
        kept = keep != 0
        before = positions[None, :] < positions[:, None]

        def rank_of(member, label):
            same = (label[:, None] == label[None, :]) & member[None, :] & before
            return jnp.sum(same.astype(jnp.int32), axis=1)

        over = kept & (rank_of(kept, served) >= direct)
        left = over & (rank_of(over, served // 2) >= pooled)
        rows = (tokens.astype(jnp.float32) * scale[:, None]).astype(jnp.bfloat16)
        lanes = 3 * spill
        to_right = host == (expert_id + 1) % experts
        lane_index = jnp.where(
            is_spill, spill + level + jnp.where(to_right, 0, spill), token_slot
        )
        cell_index = served * lanes + lane_index
        source_row = jnp.zeros((experts * lanes,), jnp.int32).at[cell_index].set(positions)
        outgoing = rows[source_row].reshape(experts, lanes, width)
        incoming = lax.all_to_all(outgoing, "expert", split_axis=0, concat_axis=0, tiled=True)
        answers = lax.all_to_all(
            expert_ffn(incoming, *weights), "expert", split_axis=0, concat_axis=0, tiled=True
        )
        rest = answers.reshape(-1, width)[cell_index].astype(jnp.float32)
        gate = jnp.dot(tokens, shared_gate, preferred_element_type=jnp.float32)
        up = jnp.dot(tokens, shared_up, preferred_element_type=jnp.float32)
        hidden = (jax.nn.silu(gate) * up).astype(jnp.bfloat16)
        common = jnp.dot(hidden, shared_down, preferred_element_type=jnp.float32)
        return jnp.where(left[:, None], (common + rest).astype(jnp.bfloat16), out)

    return lax.cond(need[0, 0] > 0, some_left, lambda: hand_over(out))


def body(
    tokens,
    router_logit,
    expert_id,
    token_slot,
    keep,
    overflow_host,
    expert_gate,
    expert_up,
    expert_down,
    shared_gate,
    shared_up,
    shared_down,
):
    experts = lax.axis_size("expert")
    dps = lax.axis_size("dp")
    groups = experts // 2
    tok_count, model_width = tokens.shape
    slot_count = 2 * tok_count // experts
    home_count = slot_count // 2
    spill_count = slot_count - home_count
    direct = max(1, 3 * home_count // 4)
    pooled = home_count
    narrow = shared_gate.shape[1] + experts <= 128 and spill_count == home_count
    even = dps in (2, 4, 8) and model_width % (2 * dps * 128) == 0
    if groups == 4 and even and narrow:
        args = (tokens, router_logit, expert_id, token_slot, keep, overflow_host)
        args += (expert_gate, expert_up, expert_down, shared_gate, shared_up, shared_down)
        return slab_body(direct, pooled, args)
    w_gate, w_up, w_down = expert_gate[0], expert_up[0], expert_down[0]
    token_scale = jax.nn.sigmoid(router_logit) * keep.astype(jnp.float32)
    positions = jnp.arange(tok_count, dtype=jnp.int32)
    is_spill = token_slot >= home_count
    spill_level = jnp.maximum(token_slot - home_count, 0)
    table_index = expert_id * spill_count + spill_level
    table_ids = jnp.arange(experts * spill_count, dtype=jnp.int32)
    host_expert = jnp.sum(
        jnp.where(table_index[:, None] == table_ids[None, :], overflow_host.reshape(1, -1), 0),
        axis=1,
    )
    served = jnp.where(is_spill, host_expert, expert_id)
    kept = keep != 0
    before = positions[None, :] < positions[:, None]

    def rank_of(member, label):
        same = (label[:, None] == label[None, :]) & member[None, :] & before
        return jnp.sum(same.astype(jnp.int32), axis=1)

    direct_rank = rank_of(kept, served)
    over = kept & (direct_rank >= direct)
    pool_rank = rank_of(over, served // 2)
    left = over & (pool_rank >= pooled)
    home_cell = jnp.where(kept & ~over, served * direct + direct_rank, -1)
    pool_cell = jnp.where(over & ~left, (served // 2) * pooled + pool_rank, -1)
    home_ids = jnp.arange(experts * direct, dtype=jnp.int32)
    pool_ids = jnp.arange(groups * pooled, dtype=jnp.int32)
    home_pick = (home_ids[:, None] == home_cell[None, :]).astype(jnp.bfloat16)
    pool_pick = (pool_ids[:, None] == pool_cell[None, :]).astype(jnp.bfloat16)
    unserved = jnp.broadcast_to(jnp.max(left.astype(jnp.int32)), (8, 128))
    side = jnp.sum(
        jnp.where(pool_ids[:, None] == pool_cell[None, :], (served % 2)[None, :], 0), axis=1
    )
    side_out = jnp.broadcast_to(side.astype(jnp.float32)[:, None], (groups * pooled, 128))
    home_ret, pool_ret, shared_hidden, unserved_all = routed_exchange(
        home_pick.reshape(experts, direct, tok_count),
        pool_pick.reshape(groups, pooled, tok_count),
        side_out.reshape(groups, pooled, 128),
        unserved,
        token_scale[:, None],
        tokens,
        w_gate,
        w_up,
        w_down,
        shared_gate.T,
        shared_up.T,
    )

    def combined():
        home_back = (home_cell[:, None] == home_ids[None, :]).astype(jnp.bfloat16)
        pool_back = (pool_cell[:, None] == pool_ids[None, :]).astype(jnp.bfloat16)
        pick = jnp.concatenate([home_back, pool_back, shared_hidden], axis=1)
        source = jnp.concatenate(
            [home_ret.reshape(-1, model_width), pool_ret.reshape(-1, model_width), shared_down],
            axis=0,
        )
        return jnp.dot(pick, source, preferred_element_type=jnp.float32)

    def all_served():
        return combined().astype(jnp.bfloat16)

    def some_left():
        rows = (tokens.astype(jnp.float32) * token_scale[:, None]).astype(jnp.bfloat16)
        lanes = home_count + 2 * spill_count
        to_right = host_expert == (expert_id + 1) % experts
        lane_index = jnp.where(
            is_spill,
            home_count + spill_level + jnp.where(to_right, 0, spill_count),
            token_slot,
        )
        cell_index = served * lanes + lane_index
        source_row = jnp.zeros((experts * lanes,), jnp.int32).at[cell_index].set(positions)
        outgoing = rows[source_row].reshape(experts, lanes, model_width)
        incoming = lax.all_to_all(outgoing, "expert", split_axis=0, concat_axis=0, tiled=True)
        answers = lax.all_to_all(
            expert_ffn(incoming, w_gate, w_up, w_down),
            "expert",
            split_axis=0,
            concat_axis=0,
            tiled=True,
        )
        rest = answers.reshape(-1, model_width)[cell_index].astype(jnp.float32)
        return (combined() + jnp.where(left[:, None], rest, 0.0)).astype(jnp.bfloat16)

    return lax.cond(unserved_all[0, 0] > 0, some_left, all_served)


def solution(mesh):
    return jax.shard_map(
        body,
        mesh=mesh,
        in_specs=(
            P(("dp", "expert"), None),
            P(("dp", "expert")),
            P(("dp", "expert")),
            P(("dp", "expert")),
            P(("dp", "expert")),
            P(),
            P("expert", None, None),
            P("expert", None, None),
            P("expert", None, None),
            P(),
            P(),
            P(),
        ),
        out_specs=P(("dp", "expert"), None),
        check_vma=False,
    )
```

```python
import functools

import jax
import jax.numpy as jnp
from jax import lax
from jax.experimental import pallas as pl
from jax.experimental.pallas import tpu as pltpu
from jax.sharding import PartitionSpec as P

MESH = pl.DeviceIdType.MESH


def expert_ffn(inputs, w_gate, w_up, w_down):
    flat_rows = inputs.reshape(-1, inputs.shape[-1])
    gate_out = jnp.dot(flat_rows, w_gate, preferred_element_type=jnp.float32)
    up_out = jnp.dot(flat_rows, w_up, preferred_element_type=jnp.float32)
    hidden = (jax.nn.silu(gate_out) * up_out).astype(jnp.bfloat16)
    result = jnp.dot(hidden, w_down, preferred_element_type=jnp.float32).astype(jnp.bfloat16)
    return result.reshape(inputs.shape)


def flip(index, step, count):
    out, bit = 0, 1
    while bit < count:
        out = out + bit * lax.rem(index // bit + step // bit, 2)
        bit *= 2
    return out


def moe_kernel(
    dps,
    experts,
    groups,
    home_pick,
    pool_pick,
    side_out,
    need_ref,
    scale_ref,
    tok_ref,
    wg_hbm,
    wu_hbm,
    wd_hbm,
    sg_ref,
    su_ref,
    home_ret,
    pool_ret,
    shared_ref,
    need_max,
    need_all,
    routed_in,
    home_out,
    pool_out,
    home_in,
    home_res,
    pool_in,
    pool_res,
    pool_part,
    pool_comb,
    side_in,
    wg,
    wu,
    wd,
    w_sem,
    own_sem,
    ns_sem,
    nr_sem,
    hs_sem,
    hr_sem,
    rs_sem,
    rr_sem,
    zs_sem,
    zr_sem,
    ms_sem,
    mr_sem,
    xs_sem,
    xr_sem,
    ps_sem,
    pr_sem,
    cs_sem,
    cr_sem,
):
    my_dp = lax.axis_index("dp")
    e = lax.axis_index("expert")
    g = e // 2
    p = e - 2 * g
    partner = e + 1 - 2 * p
    total = dps * experts
    me = my_dp * experts + e

    barrier = pltpu.get_barrier_semaphore()

    @pl.loop(1, total)
    def _(k):
        there = lax.rem(me + k, total)
        pl.semaphore_signal(
            barrier,
            inc=1,
            device_id={"dp": there // experts, "expert": lax.rem(there, experts)},
            device_id_type=MESH,
        )

    weights = [
        pltpu.make_async_copy(a, b, w_sem.at[i])
        for i, (a, b) in enumerate(((wg_hbm, wg), (wu_hbm, wu), (wd_hbm, wd)))
    ]
    own = [
        pltpu.make_async_copy(home_out.at[e], home_in.at[e], own_sem.at[0]),
        pltpu.make_async_copy(pool_out.at[g], pool_in.at[0, g], own_sem.at[1]),
        pltpu.make_async_copy(side_out.at[g], side_in.at[g], own_sem.at[2]),
        pltpu.make_async_copy(need_ref, need_all.at[me], own_sem.at[3]),
    ]

    def remote(src, dst, send, recv, to):
        return pltpu.make_async_remote_copy(
            src_ref=src,
            dst_ref=dst,
            send_sem=send,
            recv_sem=recv,
            device_id={"expert": to},
            device_id_type=MESH,
        )

    def n_copy(k):
        there = lax.rem(me + k, total)
        return pltpu.make_async_remote_copy(
            src_ref=need_ref,
            dst_ref=need_all.at[me],
            send_sem=ns_sem.at[k],
            recv_sem=nr_sem.at[k],
            device_id={"dp": there // experts, "expert": lax.rem(there, experts)},
            device_id_type=MESH,
        )

    def z_copy(k):
        to = flip(g, k, groups)
        return remote(pool_out.at[to], pool_in.at[0, g], zs_sem.at[k], zr_sem.at[k], 2 * to + p)

    def m_copy(k):
        to = flip(g, k, groups)
        return remote(side_out.at[to], side_in.at[g], ms_sem.at[k], mr_sem.at[k], 2 * to + p)

    def h_copy(k):
        to = flip(e, k, experts)
        return remote(home_out.at[to], home_in.at[e], hs_sem.at[k], hr_sem.at[k], to)

    def x_copy(k):
        origin = flip(g, k, groups)
        return remote(
            pool_in.at[0, origin],
            pool_in.at[1, flip(g, k, groups)],
            xs_sem.at[k],
            xr_sem.at[k],
            partner,
        )

    def p_copy(k):
        origin = flip(g, k, groups)
        return remote(
            pool_res.at[origin], pool_part.at[origin], ps_sem.at[k], pr_sem.at[k], partner
        )

    def c_copy(k):
        origin = flip(g, k, groups)
        return remote(
            pool_comb.at[origin], pool_ret.at[g], cs_sem.at[k], cr_sem.at[k], 2 * origin + p
        )

    def r_copy(k):
        origin = flip(e, k, experts)
        return remote(home_res.at[origin], home_ret.at[e], rs_sem.at[k], rr_sem.at[k], origin)

    def rows_of(pick):
        return jnp.dot(pick, routed_in[...], preferred_element_type=jnp.float32).astype(jnp.bfloat16)

    routed_in[...] = (tok_ref[...].astype(jnp.float32) * scale_ref[...]).astype(jnp.bfloat16)

    pl.semaphore_wait(barrier, total - 1)

    @pl.loop(1, groups + 1)
    def _(i):
        k = groups - i
        to = flip(g, k, groups)
        pool_out[to] = rows_of(pool_pick[to])

        @pl.when(i > 1)
        def _():
            z_copy(k + 1).start()
            m_copy(k + 1).start()

    @pl.loop(1, experts + 1)
    def _(i):
        k = experts - i
        to = flip(e, k, experts)
        home_out[to] = rows_of(home_pick[to])

        @pl.when(i > 1)
        def _():
            h_copy(k + 1).start()

    for copy in own:
        copy.start()
    for copy in weights:
        copy.start()

    @pl.loop(1, total)
    def _(k):
        n_copy(k).start()

    for copy in own:
        copy.wait()
    x_copy(0).start()

    tok = tok_ref[...]
    last = (((1,), (1,)), ((), ()))
    shared_gate = lax.dot_general(tok, sg_ref[...], last, preferred_element_type=jnp.float32)
    shared_up = lax.dot_general(tok, su_ref[...], last, preferred_element_type=jnp.float32)
    shared_ref[...] = (jax.nn.silu(shared_gate) * shared_up).astype(jnp.bfloat16)

    for copy in weights:
        copy.wait()

    def ffn(x):
        gate_out = jnp.dot(x, wg[...], preferred_element_type=jnp.float32)
        up_out = jnp.dot(x, wu[...], preferred_element_type=jnp.float32)
        hidden = (jax.nn.silu(gate_out) * up_out).astype(jnp.bfloat16)
        return jnp.dot(hidden, wd[...], preferred_element_type=jnp.float32).astype(jnp.bfloat16)

    home_res[e] = ffn(home_in[e])
    own_ret = pltpu.make_async_copy(home_res.at[e], home_ret.at[e], own_sem.at[0])
    own_ret.start()

    @pl.loop(1, groups)
    def _(i):
        k = groups - i
        z_copy(k).wait_recv()
        x_copy(k).start()

    def home_block(i):
        k = experts - i
        origin = flip(e, k, experts)
        h_copy(k).wait_recv()
        home_res[origin] = ffn(home_in[origin])
        r_copy(k).start()

    @pl.loop(1, groups + 1)
    def _(i):
        k = groups - i
        origin = flip(g, k, groups)
        x_copy(k).wait_recv()
        pool_res[origin] = ffn(pool_in[1, origin])
        p_copy(k).start()

    @pl.loop(1, groups + 1)
    def _(i):
        k = groups - i
        origin = flip(g, k, groups)
        mine = ffn(pool_in[0, origin])
        p_copy(k).wait_recv()

        @pl.when(k > 0)
        def _():
            m_copy(k).wait_recv()

        here = jnp.abs(side_in[origin][:, :1] - p.astype(jnp.float32)) < 0.5
        pool_comb[origin] = jnp.where(here, mine, pool_part[origin])

        @pl.when(k > 0)
        def _():
            c_copy(k).start()

    own_back = pltpu.make_async_copy(pool_comb.at[g], pool_ret.at[g], own_sem.at[1])
    own_back.start()

    pl.loop(1, experts)(home_block)

    @pl.loop(0, groups)
    def _(k):
        x_copy(k).wait_send()
        p_copy(k).wait_send()

    @pl.loop(1, groups)
    def _(k):
        z_copy(k).wait_send()
        m_copy(k).wait_send()
        c_copy(k).wait()

    @pl.loop(1, total)
    def _(k):
        n_copy(k).wait()

    @pl.loop(1, experts)
    def _(k):
        h_copy(k).wait_send()
        r_copy(k).wait()

    own_ret.wait()
    own_back.wait()
    need_max[...] = jnp.max(need_all[...], axis=0)


def routed_exchange(
    home_pick, pool_pick, side_out, need, scale, tokens, w_gate, w_up, w_down, shared_gate, shared_up
):
    dps, experts = lax.axis_size("dp"), lax.axis_size("expert")
    groups = pool_pick.shape[0]
    width = tokens.shape[1]
    home_shape, pool_shape = home_pick.shape[:2] + (width,), pool_pick.shape[:2] + (width,)
    bf16 = jnp.bfloat16
    vmem = pl.BlockSpec(memory_space=pltpu.VMEM)
    anywhere = pl.BlockSpec(memory_space=pl.ANY)
    dma = pltpu.SemaphoreType.DMA
    return pl.pallas_call(
        functools.partial(moe_kernel, dps, experts, groups),
        out_shape=(
            jax.ShapeDtypeStruct(home_shape, bf16),
            jax.ShapeDtypeStruct(pool_shape, bf16),
            jax.ShapeDtypeStruct((tokens.shape[0], shared_gate.shape[0]), bf16),
            jax.ShapeDtypeStruct(need.shape, need.dtype),
        ),
        in_specs=[vmem] * 6 + [anywhere] * 3 + [vmem] * 2,
        out_specs=(vmem,) * 4,
        scratch_shapes=[
            pltpu.VMEM((dps * experts,) + need.shape, need.dtype),
            pltpu.VMEM(tokens.shape, bf16),
            pltpu.VMEM(home_shape, bf16),
            pltpu.VMEM(pool_shape, bf16),
            pltpu.VMEM(home_shape, bf16),
            pltpu.VMEM(home_shape, bf16),
            pltpu.VMEM((2,) + pool_shape, bf16),
            pltpu.VMEM(pool_shape, bf16),
            pltpu.VMEM(pool_shape, bf16),
            pltpu.VMEM(pool_shape, bf16),
            pltpu.VMEM(side_out.shape, jnp.float32),
            pltpu.VMEM(w_gate.shape, bf16),
            pltpu.VMEM(w_up.shape, bf16),
            pltpu.VMEM(w_down.shape, bf16),
            dma((3,)),
            dma((4,)),
        ]
        + [dma((dps * experts,))] * 2
        + [dma((experts,))] * 4
        + [dma((groups,))] * 10,
        compiler_params=pltpu.CompilerParams(
            collective_id=0, has_side_effects=True, vmem_limit_bytes=60 * 1024 * 1024
        ),
        name="moe",
    )(home_pick, pool_pick, side_out, need, scale, tokens, w_gate, w_up, w_down, shared_gate, shared_up)


def split_columns(total, step=128):
    out, at = [], 0
    while at < total:
        out.append((at, min(step, total - at)))
        at += step
    return out


def slab_kernel(
    dps,
    experts,
    groups,
    direct,
    pooled,
    id_ref,
    slot_ref,
    keep_ref,
    logit_ref,
    table_ref,
    tok_hbm,
    wg_hbm,
    wu_hbm,
    wd_hbm,
    sg_hbm,
    su_hbm,
    sd_hbm,
    out_ref,
    need_max,
    tok_ref,
    sg_ref,
    su_ref,
    need_part,
    need_all,
    back,
    shared_slab,
    home_out,
    pool_out,
    home_in,
    pool_in,
    res,
    ret,
    wg,
    wu,
    slab,
    sel_all,
    h_all,
    spread,
    stage,
    in_sem,
    w_sem,
    own_sem,
    ns_sem,
    nr_sem,
    ds_sem,
    dr_sem,
    hs_sem,
    hr_sem,
    rs_sem,
    rr_sem,
    zs_sem,
    zr_sem,
    xs_sem,
    xr_sem,
    ls_sem,
    lr_sem,
    gs_sem,
    gr_sem,
    os_sem,
    or_sem,
    vs_sem,
    vr_sem,
    ss_sem,
    sr_sem,
):
    my_dp = lax.axis_index("dp")
    e = lax.axis_index("expert")
    g = e // 2
    p = e - 2 * g
    partner = e + 1 - 2 * p
    members = 2 * dps
    j = p * dps + my_dp
    half = groups // 2
    mate = flip(g, 1, groups)
    far_mid = jnp.where(g < half, half, half - 1)
    far_end = flip(far_mid, 1, groups)
    is_mid = (g == half) | (g == half - 1)
    mid = is_mid.astype(jnp.int32)
    rows, width = tok_ref.shape
    hid = wg.shape[1]
    mix = sg_ref.shape[0]
    spill = table_ref.shape[1]
    base = (direct + 7) // 8 * 8
    stride = base + pooled
    ncols = slab.shape[3]
    chunks = split_columns(ncols)

    barrier = pltpu.get_barrier_semaphore()

    @pl.loop(1, experts)
    def _(k):
        there = {"expert": flip(e, k, experts)}
        pl.semaphore_signal(barrier, inc=1, device_id=there, device_id_type=MESH)

    def peer(k):
        m = flip(j, k, members)
        return m, {"dp": lax.rem(m, dps), "expert": 2 * g + m // dps}

    strangers = [k for k in range(1, members) if k != dps]
    for k in strangers:
        pl.semaphore_signal(barrier, inc=1, device_id=peer(k)[1], device_id_type=MESH)

    def columns(member, at=0, count=ncols):
        return pl.ds(pl.multiple_of(member * ncols + at, 128), count)

    weights = [
        pltpu.make_async_copy(a, b, w_sem.at[i])
        for i, (a, b) in enumerate(((wg_hbm, wg), (wu_hbm, wu)))
    ]
    own_slab = pltpu.make_async_copy(wd_hbm.at[:, columns(j)], slab.at[g, p], w_sem.at[2])
    own_mix = pltpu.make_async_copy(
        sd_hbm.at[:, columns(j)], shared_slab.at[pl.ds(0, mix)], own_sem.at[2]
    )
    own = [
        pltpu.make_async_copy(home_out.at[e], home_in.at[e], own_sem.at[0]),
        pltpu.make_async_copy(pool_out.at[g], pool_in.at[g, 0], own_sem.at[1]),
    ]

    def remote(src, dst, send, recv, to):
        return pltpu.make_async_remote_copy(
            src_ref=src,
            dst_ref=dst,
            send_sem=send,
            recv_sem=recv,
            device_id=to,
            device_id_type=MESH,
        )

    def n_copy(k):
        there = {"expert": flip(e, k, experts)}
        return remote(need_part.at[e], need_part.at[e], ns_sem.at[k], nr_sem.at[k], there)

    def d_copy(k):
        there = {"dp": flip(my_dp, k, dps)}
        part = need_all.at[my_dp]
        return remote(part, part, ds_sem.at[k], dr_sem.at[k], there)

    def z_copy(k):
        to = flip(g, k, groups)
        there = {"expert": 2 * to + p}
        return remote(pool_out.at[to], pool_in.at[g, 0], zs_sem.at[k], zr_sem.at[k], there)

    def h_copy(k):
        to = flip(e, k, experts)
        return remote(home_out.at[to], home_in.at[e], hs_sem.at[k], hr_sem.at[k], {"expert": to})

    def x_copy(k):
        origin = flip(g, k, groups)
        return remote(
            pool_in.at[origin, 0],
            pool_in.at[flip(g, k, groups), 1],
            xs_sem.at[k],
            xr_sem.at[k],
            {"expert": partner},
        )

    def r_copy(k):
        origin = flip(e, k, experts)
        return remote(res.at[origin], ret.at[e], rs_sem.at[k], rr_sem.at[k], {"expert": origin})

    def l_copy(k):
        return remote(sel_all.at[j], sel_all.at[j], ls_sem.at[k], lr_sem.at[k], peer(k)[1])

    def g_copy(k):
        block, there = (j, peer(k)[1]) if k == 1 or k % 2 == 0 else (peer(k - 1)[0], peer(1)[1])
        return remote(h_all.at[block], h_all.at[block], gs_sem.at[k], gr_sem.at[k], there)

    def o_copy(k, c):
        at, count = chunks[c]
        m, there = peer(k)
        return remote(
            stage.at[m, :, pl.ds(at, count)],
            out_ref.at[:, columns(j, at, count)],
            os_sem.at[k, c],
            or_sem.at[k, c],
            there,
        )

    def v_copy():
        j_there = (1 - p) * dps + my_dp
        return remote(
            wd_hbm.at[:, columns(j_there)],
            slab.at[g, p],
            vs_sem.at[0],
            vr_sem.at[0],
            {"expert": partner},
        )

    def s_copy(block, c, slot, to):
        at, count = chunks[c]
        part = slab.at[block, :, :, pl.ds(at, count)]
        return remote(part, part, ss_sem.at[slot, c], sr_sem.at[block, c], {"expert": 2 * to + p})

    inputs = [
        pltpu.make_async_copy(a, b, in_sem.at[i])
        for i, (a, b) in enumerate(((tok_hbm, tok_ref), (sg_hbm, sg_ref), (su_hbm, su_ref)))
    ]
    for copy in inputs:
        copy.start()
    own_slab.start()
    own_mix.start()
    for copy in weights:
        copy.start()

    bf16 = jnp.bfloat16

    def steps(count):
        return lax.broadcasted_iota(jnp.int32, (count, rows), 0)

    def marks_of(count, label):
        return jnp.where(steps(count) == label, 1.0, 0.0)

    with jax.named_scope("routing"):
        ident, slot = id_ref[...], slot_ref[...]
        kept = keep_ref[...] != 0
        scale = jax.nn.sigmoid(logit_ref[...]) * keep_ref[...].astype(jnp.float32)
        levels = marks_of(spill, jnp.maximum(slot - spill, 0)).astype(bf16)
        table = table_ref[...].astype(jnp.float32).astype(bf16)
        hosts = jnp.dot(table, levels, preferred_element_type=jnp.float32)
        host = jnp.sum(hosts * marks_of(experts, ident), axis=0, keepdims=True)
        served = jnp.where(slot >= spill, host.astype(jnp.int32), ident)
        order = lax.broadcasted_iota(jnp.int32, (rows, rows), 1)
        earlier = jnp.where(steps(rows) < order, 1.0, 0.0).astype(bf16)

        def rank_of(count, label):
            marks = marks_of(count, label)
            counts = jnp.dot(marks.astype(bf16), earlier, preferred_element_type=jnp.float32)
            return jnp.sum(marks * counts, axis=0, keepdims=True).astype(jnp.int32)

        direct_rank = rank_of(experts, jnp.where(kept, served, -1))
        over = kept & (direct_rank >= direct)
        pool_rank = rank_of(groups, jnp.where(over, served // 2, -1))
        left = over & (pool_rank >= pooled)
        home_cell = jnp.where(kept & (direct_rank < direct), served * direct + direct_rank, -1)
        pool_cell = jnp.where(
            over & (pool_rank < pooled), (served // 2) * pooled + pool_rank, -1
        )
        placed = kept & ((direct_rank < direct) | (pool_rank < pooled))

    def rows_of(cell, first, count):
        pick = marks_of(count, cell - first)
        factor = jnp.sum(pick * scale, axis=1, keepdims=True)
        chosen = jnp.dot(pick.astype(bf16), tok_ref[...], preferred_element_type=jnp.float32)
        return (chosen * factor).astype(bf16)

    with jax.named_scope("tok_wait"):
        inputs[0].wait()

    def pack_pool(k):
        to = flip(g, k, groups)
        with jax.named_scope("pack_pool"):
            pool_out[to] = rows_of(pool_cell, to * pooled, pooled)

    pack_pool(3 - mid)
    pack_pool(2 + mid)

    with jax.named_scope("barrier"):
        pl.semaphore_wait(barrier, experts - 1 + len(strangers))

    z_copy(3 - mid).start()
    z_copy(2 + mid).start()
    pack_pool(1)
    z_copy(1).start()
    pack_pool(0)
    v_copy().start()

    @pl.loop(0, experts)
    def _(i):
        to = flip(e, experts - 1 - i, experts)
        with jax.named_scope("pack_home"):
            home_out[to] = rows_of(home_cell, to * direct, direct)

    with jax.named_scope("shared"):
        inputs[1].wait()
        inputs[2].wait()
        tok = tok_ref[...]
        last = (((1,), (1,)), ((), ()))
        shared_gate = lax.dot_general(tok, sg_ref[...], last, preferred_element_type=jnp.float32)
        shared_up = lax.dot_general(tok, su_ref[...], last, preferred_element_type=jnp.float32)
        lanes = sel_all.shape[2]
        marks = jnp.transpose(marks_of(lanes, jnp.where(placed, served + mix, -1)))
        sel_all[j] = marks.astype(bf16)
        sel_all[j, :, :mix] = (jax.nn.silu(shared_gate) * shared_up).astype(bf16)

    with jax.named_scope("tables"):
        res[...] = jnp.zeros_like(res)
        shared_slab[mix:, :] = jnp.zeros((lanes - mix, ncols), bf16)
        spot = jnp.where(direct_rank < direct, direct_rank, base + pool_rank)
        cell = jnp.where(placed, served * stride + spot, -1)
        back[...] = jnp.transpose(marks_of(experts * stride, cell)).astype(bf16)
        missed = jnp.max(jnp.where(left, 1.0, 0.0), axis=1, keepdims=True)
        need_part[e] = jnp.broadcast_to(missed, need_part.shape[1:])

    for copy in own[1:]:
        copy.start()
    own[1].wait()
    x_copy(0).start()

    def pool_relay(k):
        with jax.named_scope("z_wait"):
            z_copy(k).wait_recv()
        x_copy(k).start()

    pool_relay(3 - mid)

    @pl.loop(1, experts)
    def _(i):
        h_copy(experts - i).start()

    own[0].start()
    pool_relay(1)

    @pl.loop(1, experts)
    def _(k):
        n_copy(k).start()

    @pl.loop(1, members)
    def _(k):
        l_copy(k).start()

    with jax.named_scope("own_wait"):
        own[0].wait()
        own_mix.wait()

    with jax.named_scope("slab_wait"):
        own_slab.wait()
        v_copy().wait_recv()
    for c in range(len(chunks)):
        s_copy(g, c, 0, mate).start()

    with jax.named_scope("w_wait"):
        for copy in weights:
            copy.wait()

    def hidden_of(x):
        gate_out = jnp.dot(x, wg[...], preferred_element_type=jnp.float32)
        up_out = jnp.dot(x, wu[...], preferred_element_type=jnp.float32)
        return (jax.nn.silu(gate_out) * up_out).astype(jnp.bfloat16)

    with jax.named_scope("ffn_own"):
        res[e, :direct, :] = hidden_of(home_in[e])

    pool_relay(2 + mid)

    @pl.loop(0, groups)
    def _(i):
        k = jnp.where(i == 0, 0, jnp.where(i == 1, 3 - mid, jnp.where(i == 2, 1, 2 + mid)))
        origin = flip(g, k, groups)
        with jax.named_scope("x_wait"):
            x_copy(k).wait_recv()
        with jax.named_scope("ffn_pool"):
            both = hidden_of(pool_in[origin].reshape(2 * pooled, width))
            res[2 * origin + p, base : base + pooled, :] = both[:pooled]
            res[2 * origin + 1 - p, base : base + pooled, :] = both[pooled:]

    own_ret = pltpu.make_async_copy(res.at[e], ret.at[e], own_sem.at[0])
    own_ret.start()

    def home_block(k):
        origin = flip(e, k, experts)
        with jax.named_scope("h_wait"):
            h_copy(k).wait_recv()
        with jax.named_scope("ffn_home"):
            res[origin, :direct, :] = hidden_of(home_in[origin])
        r_copy(k).start()

    @pl.loop(1, experts)
    def _(i):
        home_block(jnp.where(i < experts // 2, experts // 2 - i, experts + experts // 2 - 1 - i))

    def far_start(*which):
        for c in which:
            s_copy(g, c, 1, far_mid).start()

    far_start(0)

    def relay(c):
        @pl.when(is_mid)
        def _():
            if c < len(chunks):
                with jax.named_scope("slab_relay"):
                    for slot, block in ((2, far_mid), (3, far_end)):
                        copy = s_copy(block, c, slot, mate)
                        copy.wait_recv()
                        copy.start()

    own_ret.wait()

    with jax.named_scope("ret_wait"):

        @pl.loop(1, experts)
        def _(i):
            r_copy(experts - i).wait_recv()

    far_start(*range(1, min(2, len(chunks))))

    with jax.named_scope("find"):
        found = jnp.dot(
            back[...], ret[...].reshape(-1, hid), preferred_element_type=jnp.float32
        )
        h_all[j] = found.astype(jnp.bfloat16)

    for k in [*range(members - 2, 0, -2), 1]:
        g_copy(k).start()

    def expand(m):
        values = h_all[m]
        marks = sel_all[m].astype(jnp.float32)
        for x in range(experts):
            mark = marks[:, mix + x : mix + x + 1] > 0.5
            spread[m, :, x * hid : (x + 1) * hid] = jnp.where(mark, values, jnp.zeros_like(values))

    def slab_arrive(c):
        s_copy(mate, c, 0, mate).wait_recv()

        @pl.when(jnp.logical_not(is_mid))
        def _():
            for block in (far_mid, far_end):
                s_copy(block, c, 2, mate).wait_recv()

    def project(m, c):
        at, count = chunks[c]
        w = slab[:, :, :, at : at + count].reshape(experts * hid, count)
        y = jnp.dot(spread[m], w, preferred_element_type=jnp.float32).astype(bf16)
        common = shared_slab[:, at : at + count]
        common = jnp.dot(sel_all[m], common, preferred_element_type=jnp.float32)
        stage[m, :, at : at + count] = (y.astype(jnp.float32) + common).astype(bf16)

    with jax.named_scope("expand"):
        expand(j)

    def hidden_arrive(k):
        with jax.named_scope("g_wait"):
            l_copy(k).wait_recv()
            g_copy(k).wait_recv()
        if k % 2 == 0:
            g_copy(k + 1).start()
        with jax.named_scope("expand"):
            expand(peer(k)[0])

    hidden_arrive(1)
    for k in range(2, members, 2):
        hidden_arrive(k)
    relay(0)
    far_start(*range(2, min(3, len(chunks))))
    for k in range(3, members, 2):
        hidden_arrive(k)
    relay(1)

    @pl.loop(1, experts)
    def _(k):
        n_copy(k).wait_recv()

    need_all[my_dp] = jnp.max(need_part[...], axis=0)

    @pl.loop(1, dps)
    def _(k):
        d_copy(k).start()

    def own_out(c):
        at, count = chunks[c]
        return pltpu.make_async_copy(
            stage.at[j, :, pl.ds(at, count)],
            out_ref.at[:, columns(j, at, count)],
            os_sem.at[0, c],
        )

    def finish_out(c):
        @pl.loop(1, members)
        def _(k):
            with jax.named_scope("out_wait"):
                o_copy(k, c).wait()

        own_out(c).wait()

    def finish_sends():
        v_copy().wait_send()
        for c in range(len(chunks)):
            s_copy(g, c, 0, mate).wait_send()
            if c + 1 < len(chunks):
                s_copy(g, c, 1, far_mid).wait_send()

        @pl.loop(0, groups)
        def _(k):
            x_copy(k).wait_send()

        @pl.loop(1, groups)
        def _(k):
            z_copy(k).wait_send()

        @pl.loop(1, members)
        def _(k):
            l_copy(k).wait_send()

        for k in range(1, members):
            g_copy(k).wait_send()

        @pl.loop(1, experts)
        def _(k):
            n_copy(k).wait_send()
            h_copy(k).wait_send()
            r_copy(k).wait_send()

        @pl.loop(1, dps)
        def _(k):
            d_copy(k).wait()

    def finish_relays():
        s_copy(g, len(chunks) - 1, 1, far_mid).wait_send()

        @pl.when(is_mid)
        def _():
            for c in range(len(chunks)):
                for slot, block in ((2, far_mid), (3, far_end)):
                    s_copy(block, c, slot, mate).wait_send()

    for c in range(len(chunks)):
        if c == len(chunks) - 1:
            with jax.named_scope("drain"):
                finish_sends()
                for early in range(max(0, len(chunks) - 3)):
                    finish_out(early)
        with jax.named_scope("slab_arrive"):
            slab_arrive(c)

        def send_out(i):
            k = members - i
            with jax.named_scope("project"):
                project(peer(k)[0], c)
            o_copy(k, c).start()

        pl.loop(1, members // 2)(send_out)
        if c < 2:
            far_start(*range(3 + c, min(4 + c, len(chunks)) if c == 0 else len(chunks)))
        pl.loop(members // 2, members)(send_out)

        project(j, c)
        own_out(c).start()
        relay(c + 2)

    finish_relays()

    for c in range(max(0, len(chunks) - 3), len(chunks)):
        finish_out(c)

    need_max[0, 0] = jnp.max(need_all[...])


def slab_exchange(
    direct, pooled, expert_id, token_slot, keep, router_logit, table, tokens, weights, shared
):
    dps, experts = lax.axis_size("dp"), lax.axis_size("expert")
    groups = experts // 2
    rows, width = tokens.shape
    hid = weights[0].shape[1]
    members = 2 * dps
    ncols = width // members
    parts = len(split_columns(ncols))
    cell = (direct + 7) // 8 * 8 + pooled
    bf16 = jnp.bfloat16
    vmem = pl.BlockSpec(memory_space=pltpu.VMEM)
    anywhere = pl.BlockSpec(memory_space=pl.ANY)
    dma = pltpu.SemaphoreType.DMA
    return pl.pallas_call(
        functools.partial(slab_kernel, dps, experts, groups, direct, pooled),
        out_shape=(
            jax.ShapeDtypeStruct((rows, width), bf16),
            jax.ShapeDtypeStruct((1, 1), jnp.float32),
        ),
        in_specs=[vmem] * 5 + [anywhere] * 7,
        out_specs=(vmem, pl.BlockSpec(memory_space=pltpu.SMEM)),
        scratch_shapes=[
            pltpu.VMEM((rows, width), bf16),
            pltpu.VMEM(shared[0].shape[::-1], bf16),
            pltpu.VMEM(shared[1].shape[::-1], bf16),
            pltpu.VMEM((experts, 8, 128), jnp.float32),
            pltpu.VMEM((dps, 8, 128), jnp.float32),
            pltpu.VMEM((rows, experts * cell), bf16),
            pltpu.VMEM((128, ncols), bf16),
            pltpu.VMEM((experts, direct, width), bf16),
            pltpu.VMEM((groups, pooled, width), bf16),
            pltpu.VMEM((experts, direct, width), bf16),
            pltpu.VMEM((groups, 2, pooled, width), bf16),
            pltpu.VMEM((experts, cell, hid), bf16),
            pltpu.VMEM((experts, cell, hid), bf16),
            pltpu.VMEM((width, hid), bf16),
            pltpu.VMEM((width, hid), bf16),
            pltpu.VMEM((groups, 2, hid, ncols), bf16),
            pltpu.VMEM((members, rows, 128), bf16),
            pltpu.VMEM((members, rows, hid), bf16),
            pltpu.VMEM((members, rows, experts * hid), bf16),
            pltpu.VMEM((members, rows, ncols), bf16),
            dma((3,)),
            dma((3,)),
            dma((3,)),
        ]
        + [dma((experts,))] * 2
        + [dma((dps,))] * 2
        + [dma((experts,))] * 4
        + [dma((groups,))] * 4
        + [dma((members,))] * 4
        + [dma((members, parts))] * 2
        + [dma((1,))] * 2
        + [dma((4, parts)), dma((groups, parts))],
        compiler_params=pltpu.CompilerParams(
            collective_id=1, has_side_effects=True, vmem_limit_bytes=60 * 1024 * 1024
        ),
        name="slab_moe",
    )(
        *(v.reshape(1, rows) for v in (expert_id, token_slot, keep, router_logit)),
        table,
        tokens,
        *weights,
        shared[0].T,
        shared[1].T,
        shared[2],
    )


def hand_over_kernel(parts, src, dst, sem):
    rows = src.shape[0] // parts

    def copy(i):
        here = pl.ds(i * rows, rows)
        return pltpu.make_async_copy(src.at[here], dst.at[here], sem.at[i])

    for i in range(parts):
        copy(i).start()
    for i in range(parts):
        copy(i).wait()


def hand_over(values):
    parts = 4
    return pl.pallas_call(
        functools.partial(hand_over_kernel, parts),
        out_shape=jax.ShapeDtypeStruct(values.shape, values.dtype),
        in_specs=[pl.BlockSpec(memory_space=pltpu.VMEM)],
        out_specs=pl.BlockSpec(memory_space=pl.ANY),
        scratch_shapes=[pltpu.SemaphoreType.DMA((parts,))],
        compiler_params=pltpu.CompilerParams(vmem_limit_bytes=4 * 1024 * 1024),
        name="hand_over",
    )(values)


def slab_body(direct, pooled, args):
    tokens, router_logit, expert_id, token_slot, keep, table = args[:6]
    weights = tuple(w[0] for w in args[6:9])
    shared_gate, shared_up, shared_down = args[9:]
    out, need = slab_exchange(
        direct,
        pooled,
        expert_id,
        token_slot,
        keep,
        router_logit,
        table,
        tokens,
        weights,
        args[9:],
    )

    def some_left():
        experts = lax.axis_size("expert")
        count, width = tokens.shape
        spill = table.shape[1]
        scale = jax.nn.sigmoid(router_logit) * keep.astype(jnp.float32)
        positions = jnp.arange(count, dtype=jnp.int32)
        is_spill = token_slot >= spill
        level = jnp.maximum(token_slot - spill, 0)
        host = table[expert_id, level]
        served = jnp.where(is_spill, host, expert_id)
        kept = keep != 0
        before = positions[None, :] < positions[:, None]

        def rank_of(member, label):
            same = (label[:, None] == label[None, :]) & member[None, :] & before
            return jnp.sum(same.astype(jnp.int32), axis=1)

        over = kept & (rank_of(kept, served) >= direct)
        left = over & (rank_of(over, served // 2) >= pooled)
        rows = (tokens.astype(jnp.float32) * scale[:, None]).astype(jnp.bfloat16)
        lanes = 3 * spill
        to_right = host == (expert_id + 1) % experts
        lane_index = jnp.where(
            is_spill, spill + level + jnp.where(to_right, 0, spill), token_slot
        )
        cell_index = served * lanes + lane_index
        source_row = jnp.zeros((experts * lanes,), jnp.int32).at[cell_index].set(positions)
        outgoing = rows[source_row].reshape(experts, lanes, width)
        incoming = lax.all_to_all(outgoing, "expert", split_axis=0, concat_axis=0, tiled=True)
        answers = lax.all_to_all(
            expert_ffn(incoming, *weights), "expert", split_axis=0, concat_axis=0, tiled=True
        )
        rest = answers.reshape(-1, width)[cell_index].astype(jnp.float32)
        gate = jnp.dot(tokens, shared_gate, preferred_element_type=jnp.float32)
        up = jnp.dot(tokens, shared_up, preferred_element_type=jnp.float32)
        hidden = (jax.nn.silu(gate) * up).astype(jnp.bfloat16)
        common = jnp.dot(hidden, shared_down, preferred_element_type=jnp.float32)
        return jnp.where(left[:, None], (common + rest).astype(jnp.bfloat16), out)

    return lax.cond(need[0, 0] > 0, some_left, lambda: hand_over(out))


def body(
    tokens,
    router_logit,
    expert_id,
    token_slot,
    keep,
    overflow_host,
    expert_gate,
    expert_up,
    expert_down,
    shared_gate,
    shared_up,
    shared_down,
):
    experts = lax.axis_size("expert")
    dps = lax.axis_size("dp")
    groups = experts // 2
    tok_count, model_width = tokens.shape
    slot_count = 2 * tok_count // experts
    home_count = slot_count // 2
    spill_count = slot_count - home_count
    direct = max(1, 3 * home_count // 4)
    pooled = home_count
    narrow = shared_gate.shape[1] + experts <= 128 and spill_count == home_count
    even = dps in (2, 4, 8) and model_width % (2 * dps * 128) == 0
    if groups == 4 and even and narrow:
        args = (tokens, router_logit, expert_id, token_slot, keep, overflow_host)
        args += (expert_gate, expert_up, expert_down, shared_gate, shared_up, shared_down)
        return slab_body(direct, pooled, args)
    w_gate, w_up, w_down = expert_gate[0], expert_up[0], expert_down[0]
    token_scale = jax.nn.sigmoid(router_logit) * keep.astype(jnp.float32)
    positions = jnp.arange(tok_count, dtype=jnp.int32)
    is_spill = token_slot >= home_count
    spill_level = jnp.maximum(token_slot - home_count, 0)
    table_index = expert_id * spill_count + spill_level
    table_ids = jnp.arange(experts * spill_count, dtype=jnp.int32)
    host_expert = jnp.sum(
        jnp.where(table_index[:, None] == table_ids[None, :], overflow_host.reshape(1, -1), 0),
        axis=1,
    )
    served = jnp.where(is_spill, host_expert, expert_id)
    kept = keep != 0
    before = positions[None, :] < positions[:, None]

    def rank_of(member, label):
        same = (label[:, None] == label[None, :]) & member[None, :] & before
        return jnp.sum(same.astype(jnp.int32), axis=1)

    direct_rank = rank_of(kept, served)
    over = kept & (direct_rank >= direct)
    pool_rank = rank_of(over, served // 2)
    left = over & (pool_rank >= pooled)
    home_cell = jnp.where(kept & ~over, served * direct + direct_rank, -1)
    pool_cell = jnp.where(over & ~left, (served // 2) * pooled + pool_rank, -1)
    home_ids = jnp.arange(experts * direct, dtype=jnp.int32)
    pool_ids = jnp.arange(groups * pooled, dtype=jnp.int32)
    home_pick = (home_ids[:, None] == home_cell[None, :]).astype(jnp.bfloat16)
    pool_pick = (pool_ids[:, None] == pool_cell[None, :]).astype(jnp.bfloat16)
    unserved = jnp.broadcast_to(jnp.max(left.astype(jnp.int32)), (8, 128))
    side = jnp.sum(
        jnp.where(pool_ids[:, None] == pool_cell[None, :], (served % 2)[None, :], 0), axis=1
    )
    side_out = jnp.broadcast_to(side.astype(jnp.float32)[:, None], (groups * pooled, 128))
    home_ret, pool_ret, shared_hidden, unserved_all = routed_exchange(
        home_pick.reshape(experts, direct, tok_count),
        pool_pick.reshape(groups, pooled, tok_count),
        side_out.reshape(groups, pooled, 128),
        unserved,
        token_scale[:, None],
        tokens,
        w_gate,
        w_up,
        w_down,
        shared_gate.T,
        shared_up.T,
    )

    def combined():
        home_back = (home_cell[:, None] == home_ids[None, :]).astype(jnp.bfloat16)
        pool_back = (pool_cell[:, None] == pool_ids[None, :]).astype(jnp.bfloat16)
        pick = jnp.concatenate([home_back, pool_back, shared_hidden], axis=1)
        source = jnp.concatenate(
            [home_ret.reshape(-1, model_width), pool_ret.reshape(-1, model_width), shared_down],
            axis=0,
        )
        return jnp.dot(pick, source, preferred_element_type=jnp.float32)

    def all_served():
        return combined().astype(jnp.bfloat16)

    def some_left():
        rows = (tokens.astype(jnp.float32) * token_scale[:, None]).astype(jnp.bfloat16)
        lanes = home_count + 2 * spill_count
        to_right = host_expert == (expert_id + 1) % experts
        lane_index = jnp.where(
            is_spill,
            home_count + spill_level + jnp.where(to_right, 0, spill_count),
            token_slot,
        )
        cell_index = served * lanes + lane_index
        source_row = jnp.zeros((experts * lanes,), jnp.int32).at[cell_index].set(positions)
        outgoing = rows[source_row].reshape(experts, lanes, model_width)
        incoming = lax.all_to_all(outgoing, "expert", split_axis=0, concat_axis=0, tiled=True)
        answers = lax.all_to_all(
            expert_ffn(incoming, w_gate, w_up, w_down),
            "expert",
            split_axis=0,
            concat_axis=0,
            tiled=True,
        )
        rest = answers.reshape(-1, model_width)[cell_index].astype(jnp.float32)
        return (combined() + jnp.where(left[:, None], rest, 0.0)).astype(jnp.bfloat16)

    return lax.cond(unserved_all[0, 0] > 0, some_left, all_served)


def solution(mesh):
    return jax.shard_map(
        body,
        mesh=mesh,
        in_specs=(
            P(("dp", "expert"), None),
            P(("dp", "expert")),
            P(("dp", "expert")),
            P(("dp", "expert")),
            P(("dp", "expert")),
            P(),
            P("expert", None, None),
            P("expert", None, None),
            P("expert", None, None),
            P(),
            P(),
            P(),
        ),
        out_specs=P(("dp", "expert"), None),
        check_vma=False,
    )
```
